32 devices in a mesh: grp: 2 (over y), gx: 4 (over z), gy: 2 (over x), gz: 2 (over core).
Axes of the slice: x: 2, y: 2, z: 4, core: 2. Of those that a mesh axis runs over, the one named last changes fastest.
Arguments:
- observed: float32 [2048, 4, 256], P(('grp', 'gx', 'gy', 'gz')), parts along dimension 0, may hold values from -12 to 12
- predicted: float32 [2048, 4, 256], P(('grp', 'gx', 'gy', 'gz')), parts along dimension 0, may hold values from -6 to 6
- coherence_mask: int32 [2048, 256], P(('grp', 'gx', 'gy', 'gz')), parts along dimension 0, may hold values 0 or 1
- block_count: int32 [2048], P(('grp', 'gx', 'gy', 'gz')), parts along dimension 0, may hold values from 64 to 256
- block_owner: int32 [2048, 1], P(('grp', 'gx', 'gy', 'gz')), parts along dimension 0, may hold values from 0 to 7; in each aligned block of 64 rows (0 to 63, 64 to 127, ...) at most 16 rows name the same one
- block_matrix_choice: int32 [2048], P(('grp', 'gx', 'gy', 'gz')), parts along dimension 0, may hold values from 0 to 31
- block_patch: int32 [2048], P(('grp', 'gx', 'gy', 'gz')), parts along dimension 0, may hold values from 0 to 31
- look_vector: float32 [4, 3], replicated, may hold values from -1 to 1
- interp_weights: bfloat16 [32, 256, 128], replicated, may hold values from -0.375 to 0.375
- depth_kernel: float32 [64], P(('grp', 'gz')), parts along dimension 0, may hold values from 0.2 to 1
- stiffness: float32 [64, 128, 256], P(('grp', 'gz'), 'gx', 'gy'), parts along dimension 0, may hold values from 0.25 to 4
Outputs:
- adjoint_field: float32 [3, 64, 128, 256], P(None, ('grp', 'gz'), 'gx', 'gy'), parts along dimension 1
- cg_residual: float32 [3, 64, 128, 256], P(None, ('grp', 'gz'), 'gx', 'gy'), parts along dimension 1
The draws below stay inside these ranges and needn't reach their ends.
There are 2 independent parts, one for each index of `grp`. The reference program is written for one: setup_inputs(seed, part) draws one part's arguments, and reference() takes and returns one part's arrays. A program takes and returns all parts, laid end to end along the dimension named above; an argument that names none is the same for every part. Nothing has to cross between parts.
Inputs may be any that keep to these rules, and one draw needn't show every extreme that they name: `block_owner`: the blocks of one device name no column tile more than 16 times; in some devices one tile is named exactly 16 times.
All inputs are finite; a program needn't handle non-finite values. No bound on the sum of `coherence_mask` on one device may be relied on, other than what follows from the above.
Results may differ from the reference program's by a relative error of at most 0.0029.
Values sent between devices are 32-bit elements; how exact they have to be, the bound alone decides.
A program may use at most 64 MiB of HBM per device.

```python
import math
import jax
import jax.numpy as jnp
import numpy as np
from jax import lax

CX = 32
CY = 128
BLK_DEV = 64
NTAB = 32
EPOCHS = 4
BPIX = 256
PATCH_X = 8
PATCH_Y = 16
ITERS = 3
NX = 128
NY = 256
NZ = 32
NBLK = 1024
CAP = 16
NPOS = 32
N_GX = 4
N_GY = 2


def draw_observed(key, part):
    rows = jnp.arange(NBLK, dtype=jnp.float32)
    spread = 1.0 + 2.0 * rows / max(NBLK - 1, 1)
    base = jax.random.truncated_normal(key, -4.0, 4.0, (NBLK, EPOCHS, BPIX), jnp.float32)
    return base * spread[:, None, None]


def place_ends(values, own_key, smallest, largest):
    dims = values.shape
    place = [jax.random.randint(jax.random.fold_in(own_key, axis), (), 0, dims[axis]) for axis in range(len(dims))]
    values = values.at[tuple(place)].set(smallest)
    longest = dims.index(max(dims))
    place[longest] = (place[longest] + 1) % dims[longest]
    return values.at[tuple(place)].set(largest)


def level_of(key, dims, split, low, largest):
    def one(dim, blocks):
        steps = jax.random.uniform(jax.random.fold_in(jax.random.fold_in(key, 6), dim), (blocks,), jnp.float32, low / len(split), largest / len(split))
        return jnp.repeat(jnp.exp(steps), dims[dim] // blocks).reshape((-1,) + (1,) * (len(dims) - dim - 1))

    level = one(*split[0])
    for cut in split[1:]:
        level = level * one(*cut)
    return level


def routed_block(rng, own, number, rows, number_of, top, reach, lean):
    ranking = jax.random.permutation(rng, number_of)
    heavy_load, ordinary = load_shares(number_of, rows * top, reach, lean, True), load_shares(number_of, rows * top, reach, lean, False)
    places = jnp.arange(number_of)

    def named(sizes, offset_by):
        used = int((sizes > 0).sum())
        fixed = max(1, used // 4)
        moved = fixed + (places - fixed + offset_by * (used - fixed)) % max(1, number_of - fixed)
        return jnp.zeros((number_of,), jnp.int32).at[ranking[jnp.where(places < fixed, places, moved)]].set(jnp.asarray(sizes, jnp.int32))

    sizes = jnp.where(number % 4 == 0, named(heavy_load, number // 4), named(ordinary, number - number // 4 - 1))
    mixed = jax.random.permutation(jax.random.fold_in(own, 3), number_of)
    giver, receiver = mixed[0:number_of // 2 * 2:2], mixed[1:number_of // 2 * 2:2]
    room = jnp.minimum(sizes[giver] - 1, reach - sizes[receiver]) // 2
    room = jnp.where((giver == ranking[0]) | (receiver == ranking[0]) | (sizes[receiver] == 0), 0, jnp.maximum(room, 0))
    moved = jax.random.randint(jax.random.fold_in(own, 4), (number_of // 2,), 0, 1 << 20) % (room + 1)
    sizes = sizes.at[giver].add(-moved).at[receiver].add(moved)
    members = jnp.searchsorted(jnp.cumsum(sizes), jnp.arange(rows * top), side="right").astype(jnp.int32)
    table = members.reshape(top, rows).T
    table = table[jax.random.permutation(jax.random.fold_in(own, 1), rows)]
    offset_by = jax.random.randint(jax.random.fold_in(own, 2), (rows, 1), 0, top)
    return jnp.take_along_axis(table, (jnp.arange(top)[None, :] + offset_by) % top, axis=1)


def load_shares(amount, total, bound, lean, full):
    portions = [(1 << 20) // math.isqrt(grade ** lean) + 1 for grade in range(1, amount + 1)]
    largest = bound if full else min(bound, max(-(-total // amount), total * portions[0] // sum(portions)))
    least = 1 if total - largest >= amount - 1 else 0
    counts, surplus = [largest] + [least] * (amount - 1), total - largest - least * (amount - 1)
    while surplus > 0:
        movable = [i for i in range(1, amount) if counts[i] < largest] or [i for i in range(1, amount) if counts[i] < bound]
        pool, budget = sum([portions[i] for i in movable]), surplus
        for i in movable:
            extra = min(bound - counts[i], max(1, budget * portions[i] // pool), surplus)
            counts[i] = counts[i] + extra
            surplus = surplus - extra
    return np.array(counts)


def noise(key, dims, deviation, bound, split=(), kind=jnp.bfloat16):
    level = level_of(key, dims, split, -0.22, 0.18) if split else 1.0
    drawn = jax.random.normal(key, dims, jnp.float32) * deviation * level
    return jnp.minimum(jnp.maximum(drawn, -bound), bound).astype(kind)


def setup_inputs(seed: int = 0, part: int = 0) -> dict:
    splits = jax.random.split(jax.random.key(seed), 12)
    part_splits = jax.random.split(jax.random.fold_in(splits[11], part), 12)
    observed = draw_observed(jax.random.fold_in(jax.random.fold_in(splits[11], part), 71), part)
    predicted = noise(part_splits[1], (NBLK, EPOCHS, BPIX), 1.0, 6.0, ((0, 16),), jnp.float32)
    coherence_mask = place_ends((jax.random.randint(part_splits[2], (NBLK, BPIX), 0, 4) < 3).astype(jnp.int32), jax.random.fold_in(part_splits[2], 1), 0, 1)
    block_count = place_ends(jax.random.randint(part_splits[3], (NBLK,), BPIX // 4, BPIX + 1), jax.random.fold_in(part_splits[3], 1), BPIX // 4, BPIX).astype(jnp.int32)
    block_owner_keys = jax.random.split(jax.random.fold_in(part_splits[4], 1), NBLK // BLK_DEV)
    block_owner_turns = jax.random.permutation(jax.random.fold_in(part_splits[4], 3), NBLK // BLK_DEV)
    block_owner = jax.vmap(lambda own, number: routed_block(jax.random.fold_in(part_splits[4], 2), own, number, BLK_DEV, N_GX * N_GY, 1, CAP, 2))(block_owner_keys, block_owner_turns).reshape((NBLK, 1))
    block_matrix_choice = place_ends(jax.random.randint(part_splits[5], (NBLK,), 0, NTAB), jax.random.fold_in(part_splits[5], 1), 0, NTAB - 1).astype(jnp.int32)
    block_patch = place_ends(jax.random.randint(part_splits[6], (NBLK,), 0, NPOS), jax.random.fold_in(part_splits[6], 1), 0, NPOS - 1).astype(jnp.int32)
    look_vector = jnp.clip(jax.random.uniform(splits[7], (EPOCHS, 3), jnp.float32, -1.0, 1.0), -1.0, 1.0)
    interp_weights = noise(splits[8], (NTAB, BPIX, PATCH_X * PATCH_Y), BPIX ** -0.5, 0.375)
    depth_kernel = jnp.clip(jnp.exp(math.log(1.0) - 1.609438 * jax.random.uniform(part_splits[9], (NZ,), jnp.float32) ** level_of(part_splits[9], (NZ,), ((0, 2),), -0.2, 0.2)), 0.2, 1.0)
    stiffness = jnp.clip(jnp.exp(math.log(4.0) - 2.7725887 * jax.random.uniform(part_splits[10], (NZ, NX, NY), jnp.float32) ** level_of(part_splits[10], (NZ, NX, NY), ((0, 2), (1, 4), (2, 2)), -0.2, 0.2)), 0.25, 4.0)
    return dict(observed=observed, predicted=predicted, coherence_mask=coherence_mask, block_count=block_count, block_owner=block_owner, block_matrix_choice=block_matrix_choice, block_patch=block_patch, look_vector=look_vector, interp_weights=interp_weights, depth_kernel=depth_kernel, stiffness=stiffness)


KAPPA = 0.5
EPS = 1e-06
SPATIAL = (1, 2, 0)

def beside_all(padded):
    total = padded[2:, 1:-1, 1:-1] + padded[:-2, 1:-1, 1:-1]
    total = total + padded[1:-1, 2:, 1:-1] + padded[1:-1, :-2, 1:-1]
    return total + padded[1:-1, 1:-1, 2:] + padded[1:-1, 1:-1, :-2]

def central(padded, axis):
    if axis == 0:
        return 0.5 * (padded[2:, 1:-1, 1:-1] - padded[:-2, 1:-1, 1:-1])
    if axis == 1:
        return 0.5 * (padded[1:-1, 2:, 1:-1] - padded[1:-1, :-2, 1:-1])
    return 0.5 * (padded[1:-1, 1:-1, 2:] - padded[1:-1, 1:-1, :-2])

def operate(field, stiffness):
    padded = jnp.pad(field, ((0, 0), (1, 1), (1, 1), (1, 1)))
    spread = central(padded[0], SPATIAL[0]) + central(padded[1], SPATIAL[1]) + central(padded[2], SPATIAL[2])
    spread_pad = jnp.pad(spread, 1)
    parts = [(6.0 + stiffness) * field[member] - beside_all(padded[member]) - KAPPA * central(spread_pad, SPATIAL[member]) for member in range(3)]
    return jnp.stack(parts)

def project(resid, look_vector):
    return jnp.einsum('ec,nep->ncp', look_vector, resid, precision=lax.Precision.HIGHEST).astype(jnp.bfloat16)

def contribute(coeffs, tables, weights):
    total = coeffs.shape[0]
    group = math.gcd(total, 64)
    coefficient_sets = coeffs.reshape(total // group, group, 3, coeffs.shape[2])
    table_groups = tables.reshape(total // group, group)

    def per_group(both_parts):
        block_coefficient_values, block_tables = both_parts
        selected_entries = jnp.take(weights, block_tables, axis=0).astype(jnp.float32)
        return jnp.einsum('aow,awv->aov', block_coefficient_values.astype(jnp.float32), selected_entries, precision=lax.Precision.HIGHEST)
    result = lax.map(per_group, (coefficient_sets, table_groups))
    return result.reshape(total, 3, weights.shape[2])

def reference(observed, predicted, coherence_mask, block_count, block_owner, block_matrix_choice, block_patch, look_vector, interp_weights, depth_kernel, stiffness):
    column = jnp.arange(BPIX, dtype=jnp.int32)
    valid = coherence_mask.astype(jnp.float32) * (column[None, :] < block_count[:, None]).astype(jnp.float32)
    resid = (predicted - observed) * valid[:, None, :]
    scale = lax.rsqrt(jnp.sum(resid * resid) / (EPOCHS * jnp.sum(valid)) + EPS)
    coeffs = project(resid, look_vector)
    sums = contribute(coeffs, block_matrix_choice, interp_weights)
    owner = block_owner[:, 0]
    tile_y = CY // PATCH_Y
    grid_x = owner // N_GY * (CX // PATCH_X) + block_patch // tile_y
    northing_grid = owner % N_GY * tile_y + block_patch % tile_y
    across_x = NX // PATCH_X
    across_y = NY // PATCH_Y
    placed = jax.ops.segment_sum(sums, (grid_x * across_y + northing_grid).astype(jnp.int32), num_segments=across_x * across_y)
    surface = placed.reshape(across_x, across_y, 3, PATCH_X, PATCH_Y).transpose(2, 0, 3, 1, 4).reshape(3, NX, NY)
    source = scale * depth_kernel[None, :, None, None] * surface[:, None, :, :]
    adjoint_field = jnp.zeros_like(source)
    cg_residual = source
    direction = source
    norm_now = jnp.sum(cg_residual * cg_residual)
    for step in range(ITERS):
        image = operate(direction, stiffness)
        alpha = norm_now / jnp.sum(direction * image)
        adjoint_field = adjoint_field + alpha * direction
        cg_residual = cg_residual - alpha * image
        norm_next = jnp.sum(cg_residual * cg_residual)
        direction = cg_residual + norm_next / norm_now * direction
        norm_now = norm_next
    return (adjoint_field, cg_residual)
```

```python
import functools

import jax
import jax.numpy as jnp
from jax import lax
from jax.experimental import pallas as pl
from jax.experimental.pallas import tpu as pltpu
from jax.sharding import PartitionSpec as P

PATCH_X = 8
PATCH_Y = 16
ITERS = 3
KAPPA = 0.5
EPS = 1e-06
SHIFT = 8.0
HX = 8
LANES = 128
MESH = pl.DeviceIdType.MESH
F32 = jnp.float32
BF16 = jnp.bfloat16


def split_dot(one_hot, values):
    high = values.astype(BF16)
    low = (values - high.astype(F32)).astype(BF16)
    return jnp.dot(one_hot, high, preferred_element_type=F32) + jnp.dot(
        one_hot, low, preferred_element_type=F32
    )


def dot_split(values, one_hot):
    high = values.astype(BF16)
    low = (values - high.astype(F32)).astype(BF16)
    return jnp.dot(high, one_hot, preferred_element_type=F32) + jnp.dot(
        low, one_hot, preferred_element_type=F32
    )


def up(a, axis):
    return pltpu.roll(a, a.shape[axis] - 1, axis)


def down(a, axis):
    return pltpu.roll(a, 1, axis)


def lane_roll(a, amount):
    amount = amount % LANES
    return a if amount == 0 else pltpu.roll(a, amount, a.ndim - 1)


def body(
    ngx, ngy, ngz, cap, epochs,
    choice, depth, partial, owner_ref, patch_ref, coeffs, weights, stiff,
    v1_out, v2_out, v3_out, surf_out, coef_out,
    sums, send, meta, recv, metarecv, part, ppk, msum, sx, sy, sc, mz,
    dext, kext, pk, pkrecv, surf, v1, v2, v3, div, fields, momsend, mom,
    a_send, a_recv, m_send, m_recv, kx_sem, ky_sem, kz_sem, dz_sem,
    h_send, sx_sem, sy_sem, sc_sem, mz_sem, r_send, r_recv, out_sem,
):
    gx = lax.axis_index("gx")
    gy = lax.axis_index("gy")
    gz = lax.axis_index("gz")
    owners = ngx * ngy
    total = owners * ngz
    me = gx * ngy + gy
    flat = me * ngz + gz
    nz, lx, ly = stiff.shape
    blocks = choice.shape[0]
    rows_x = lx + 2 * HX
    width = 2 * LANES
    places_x = lx // PATCH_X
    places_y = ly // PATCH_Y
    places = places_x * places_y
    cells = PATCH_X * PATCH_Y
    slots = owners * cap
    meta_w = meta.shape[2]

    def at(x, y, z):
        return {"gx": x, "gy": y, "gz": z}

    def peer_of(t):
        p = lax.rem(flat + t, total)
        q = p // ngz
        return p, at(q // ngy, lax.rem(q, ngy), lax.rem(p, ngz))

    barrier = pltpu.get_barrier_semaphore()

    def greet(t, carry):
        _, device = peer_of(t)
        pl.semaphore_signal(barrier, inc=1, device_id=device, device_id_type=MESH)
        return carry

    lax.fori_loop(1, total, greet, 0)

    def copy(src, dst, send_sem, recv_sem, device):
        return pltpu.make_async_remote_copy(
            src_ref=src, dst_ref=dst, send_sem=send_sem, recv_sem=recv_sem,
            device_id=device, device_id_type=MESH,
        )

    for b in range(blocks):
        table = weights[choice[b]]
        sums[b] = jnp.dot(coeffs[b], table, preferred_element_type=F32)

    for z in range(nz):
        dext[z + 6] = jnp.full((8, LANES), depth[z], F32)
    kext[4:4 + nz, HX:HX + lx, 0:LANES] = stiff[...]

    owner_col = owner_ref[...]
    patch_col = patch_ref[...]
    rows_i = lax.broadcasted_iota(jnp.int32, (blocks, blocks), 0)
    cols_i = lax.broadcasted_iota(jnp.int32, (blocks, blocks), 1)
    owner_wide = jnp.broadcast_to(owner_col, (blocks, blocks))
    owner_row = jnp.sum(jnp.where(rows_i == cols_i, owner_wide, 0), axis=0, keepdims=True)
    same = owner_wide == owner_row
    rank_row = jnp.sum(jnp.where(same & (rows_i < cols_i), 1, 0), axis=0, keepdims=True)
    rank_col = jnp.sum(jnp.where(same & (cols_i < rows_i), 1, 0), axis=1, keepdims=True)
    slot_row = owner_row * cap + rank_row
    slot_ids = lax.broadcasted_iota(jnp.int32, (slots, blocks), 0)
    select = jnp.where(slot_ids == slot_row, 1.0, 0.0).astype(BF16)
    for c in range(3):
        sent = split_dot(select, sums[:, c, :])
        send[:, c * cap:(c + 1) * cap, :] = sent.reshape(owners, cap, cells)
    lane_ids = lax.broadcasted_iota(jnp.int32, (blocks, meta_w), 1)
    ranked = jnp.where(lane_ids == rank_col + me * cap, patch_col, 0).astype(F32).astype(BF16)
    owner_ids = lax.broadcasted_iota(jnp.int32, (max(8, owners), blocks), 0)
    owner_hot = jnp.where(owner_ids == owner_row, 1.0, 0.0).astype(BF16)
    patches = jnp.dot(owner_hot, ranked, preferred_element_type=F32)
    sub_ids = lax.broadcasted_iota(jnp.int32, (8, meta_w), 0)
    extras = jnp.where(sub_ids == 1, partial[0], jnp.where(sub_ids == 2, partial[1], 0.0))
    for o in range(owners):
        line = jnp.broadcast_to(patches[o:o + 1, :], (8, meta_w))
        meta[o] = jnp.where(sub_ids == 0, line, extras)

    pl.semaphore_wait(barrier, total - 1)

    exchange = []
    for t in range(1, owners):
        o = lax.rem(me + t, owners)
        src = lax.rem(me + owners - t, owners)
        device = at(o // ngy, lax.rem(o, ngy), gz)
        data = copy(send.at[o], recv.at[me], a_send.at[t], a_recv.at[me], device)
        note = copy(meta.at[o], metarecv.at[me], m_send.at[t], m_recv.at[me], device)
        data.start()
        note.start()
        exchange.append((
            data, note,
            copy(send.at[o], recv.at[src], a_send.at[t], a_recv.at[src], device),
            copy(meta.at[o], metarecv.at[src], m_send.at[t], m_recv.at[src], device),
        ))

    def both_sides(position, count, axis, low_src, low_dst, high_src, high_dst, sem, fill):
        others = {"gx": gx, "gy": gy, "gz": gz}
        lower, upper = dict(others), dict(others)
        lower[axis] = position - 1
        upper[axis] = position + 1
        to_low = copy(low_src, high_dst, sem.at[0], sem.at[1], lower)
        to_high = copy(high_src, low_dst, sem.at[2], sem.at[3], upper)
        has_low = position > 0
        has_high = position < count - 1
        pl.when(has_low)(lambda: to_low.start())
        pl.when(has_high)(lambda: to_high.start())
        pl.when(jnp.logical_not(has_low))(lambda: fill(low_dst))
        pl.when(jnp.logical_not(has_high))(lambda: fill(high_dst))

        def finish():
            @pl.when(has_low)
            def _():
                to_low.wait_send()
                copy(low_src, low_dst, sem.at[2], sem.at[3], lower).wait_recv()

            @pl.when(has_high)
            def _():
                to_high.wait_send()
                copy(high_src, high_dst, sem.at[0], sem.at[1], upper).wait_recv()

        return finish

    def zero(ref):
        ref[...] = jnp.zeros(ref.shape, F32)

    finish_x = both_sides(
        gx, ngx, "gx",
        stiff.at[:, pl.ds(0, HX), :],
        kext.at[pl.ds(4, nz), pl.ds(0, HX), pl.ds(0, LANES)],
        stiff.at[:, pl.ds(lx - HX, HX), :],
        kext.at[pl.ds(4, nz), pl.ds(HX + lx, HX), pl.ds(0, LANES)],
        kx_sem, zero,
    )
    finish_d = both_sides(
        gz, ngz, "gz",
        dext.at[pl.ds(6, 6)], dext.at[pl.ds(0, 6)],
        dext.at[pl.ds(nz, 6)], dext.at[pl.ds(nz + 6, 6)],
        dz_sem, zero,
    )
    finish_x()
    lane1 = lax.broadcasted_iota(jnp.int32, (rows_x, LANES), 1)
    for g in range(nz // 8):
        left = jnp.zeros((rows_x, LANES), F32)
        right = jnp.zeros((rows_x, LANES), F32)
        for k in range(8):
            plane = kext[4 + 8 * g + k, :, 0:LANES]
            here = (lane1 // 16) == k
            left = jnp.where(here, lane_roll(plane, 16 * k), left)
            right = jnp.where(here, lane_roll(plane, 16 * k + 16), right)
        pk[0, g] = left
        pk[1, g] = right
    finish_y = both_sides(
        gy, ngy, "gy", pk.at[0], pkrecv.at[0], pk.at[1], pkrecv.at[1], ky_sem, zero
    )
    finish_y()
    for g in range(nz // 8):
        from_left = pkrecv[0, g]
        from_right = pkrecv[1, g]
        for k in range(8):
            kext[4 + 8 * g + k, :, LANES:width] = jnp.where(
                lane1 < 64, lane_roll(from_right, -16 * k), lane_roll(from_left, 112 - 16 * k)
            )
    finish_z = both_sides(
        gz, ngz, "gz",
        kext.at[pl.ds(4, 4)], kext.at[pl.ds(0, 4)],
        kext.at[pl.ds(nz, 4)], kext.at[pl.ds(nz + 4, 4)],
        kz_sem, zero,
    )

    recv[me] = send[me]
    metarecv[me] = meta[me]
    for data, note, data_in, note_in in exchange:
        data_in.wait_recv()
        note_in.wait_recv()

    notes = metarecv[0]
    for s in range(1, owners):
        notes = notes + metarecv[s]
    patch_row = notes[0:1, 0:slots]
    place_ids = lax.broadcasted_iota(jnp.int32, (places, slots), 0).astype(F32)
    place_hot = jnp.where(place_ids == patch_row, 1.0, 0.0).astype(BF16)
    msum[...] = notes[:, 0:LANES]
    cell_i = lax.broadcasted_iota(jnp.int32, (cells, PATCH_X * LANES), 0)
    lane_i = lax.broadcasted_iota(jnp.int32, (cells, PATCH_X * LANES), 1)
    spread = jnp.where(
        cell_i == (lane_i // LANES) * PATCH_Y + lane_i % PATCH_Y, 1.0, 0.0
    ).astype(BF16)
    wide_lane = lax.broadcasted_iota(jnp.int32, (places, PATCH_X * LANES), 1)
    wide_row = lax.broadcasted_iota(jnp.int32, (places, PATCH_X * LANES), 0)
    own_place = (wide_lane % LANES) // PATCH_Y == wide_row % places_y
    for c in range(3):
        arrived = recv[:, c * cap:(c + 1) * cap, :].reshape(slots, cells)
        placed = split_dot(place_hot, arrived)
        expanded = jnp.where(own_place, dot_split(placed, spread), 0.0)
        lines = jnp.sum(expanded.reshape(places_x, places_y, PATCH_X * LANES), axis=1)
        for i in range(PATCH_X):
            for px in range(places_x):
                row = px * PATCH_X + i
                part[c, row:row + 1, :] = lines[px:px + 1, i * LANES:(i + 1) * LANES]

    lane8 = lax.broadcasted_iota(jnp.int32, (8, LANES), 1)
    groups = lx // 8
    packs = ppk.shape[1]
    left = [jnp.zeros((8, LANES), F32)] * packs
    right = [jnp.zeros((8, LANES), F32)] * packs
    for c in range(3):
        for r in range(groups):
            k = c * groups + r
            q, kk = k // 8, k % 8
            tile = part[c, r * 8:(r + 1) * 8, :]
            here = (lane8 // 16) == kk
            left[q] = jnp.where(here, lane_roll(tile, 16 * kk), left[q])
            right[q] = jnp.where(here, lane_roll(tile, 16 * kk + 16), right[q])
    for q in range(packs):
        ppk[0, q] = left[q]
        ppk[1, q] = right[q]

    sends, receives = [], []
    number = 0
    for t in range(1, ngz):
        z = lax.rem(gz + t, ngz)
        for src, dst, sem in ((part, sc, sc_sem), (msum, mz, mz_sem)):
            out = copy(src, dst.at[gz], h_send.at[number], sem.at[gz], at(gx, gy, z))
            out.start()
            sends.append((None, out))
            receives.append((None, copy(src, dst.at[z], h_send.at[number], sem.at[z], at(gx, gy, z))))
            number += 1
    for dx in (-1, 0, 1):
        for dy in (-1, 0, 1):
            if dx == 0 and dy == 0:
                continue
            nx, ny = gx + dx, gy + dy
            there = (nx >= 0) & (nx < ngx) & (ny >= 0) & (ny < ngy)
            for z in range(ngz):
                device = at(nx, ny, z)
                if dy == 0:
                    src = part.at[:, pl.ds(lx - 8 if dx > 0 else 0, 8), :]
                    side_out, side_in = (0, 1) if dx > 0 else (1, 0)
                    out = copy(src, sx.at[side_out, gz], h_send.at[number],
                               sx_sem.at[side_out, gz], device)
                    came = copy(src, sx.at[side_in, z], h_send.at[number],
                                sx_sem.at[side_in, z], device)
                    hole = sx.at[side_in, z]
                else:
                    src = ppk.at[1 if dy > 0 else 0]
                    side_out, side_in = (0, 1) if dy > 0 else (1, 0)
                    out = copy(src, sy.at[1 - dx, side_out, gz], h_send.at[number],
                               sy_sem.at[1 - dx, side_out, gz], device)
                    came = copy(src, sy.at[1 + dx, side_in, z], h_send.at[number],
                                sy_sem.at[1 + dx, side_in, z], device)
                    hole = sy.at[1 + dx, side_in, z]
                pl.when(there)(lambda out=out: out.start())
                pl.when(jnp.logical_not(there))(lambda hole=hole: zero(hole))
                sends.append((there, out))
                receives.append((there, came))
                number += 1
    sc[gz] = part[...]
    mz[gz] = msum[...]
    finish_d()
    finish_z()
    for there, came in receives:
        if there is None:
            came.wait_recv()
        else:
            pl.when(there)(lambda came=came: came.wait_recv())

    tot = mz[0]
    for z in range(1, ngz):
        tot = tot + mz[z]
    scale = lax.rsqrt(tot[1:2, :] / (epochs * tot[2:3, :]) + EPS)

    def over_gz(ref, *index):
        value = ref[index + (0,)]
        for z in range(1, ngz):
            value = value + ref[index + (z,)]
        return value

    centre = over_gz(sc) * scale
    surf[:, HX:HX + lx, 0:LANES] = centre
    surf_out[...] = centre
    surf[:, 0:HX, 0:LANES] = over_gz(sx, 0) * scale
    surf[:, HX + lx:, 0:LANES] = over_gz(sx, 1) * scale
    edge_lane = (lane8 < 8) | (lane8 >= LANES - 8)
    for d in range(3):
        from_left = over_gz(sy, d, 0)
        from_right = over_gz(sy, d, 1)
        for c in range(3):
            for r in ((groups - 1,), range(groups), (0,))[d]:
                k = c * groups + r
                q, kk = k // 8, k % 8
                tile = jnp.where(
                    lane8 < 64, lane_roll(from_right[q], -16 * kk),
                    lane_roll(from_left[q], 112 - 16 * kk),
                )
                row = (0, HX + r * 8, HX + lx)[d]
                surf[c, row:row + 8, LANES:width] = jnp.where(edge_lane, tile * scale, 0.0)

    row_i = lax.broadcasted_iota(jnp.int32, (rows_x, width), 0)
    col_i = lax.broadcasted_iota(jnp.int32, (rows_x, width), 1)
    inside_x = ((row_i >= HX) | (gx > 0)) & ((row_i < HX + lx) | (gx < ngx - 1))
    inside_y = (col_i < LANES) | ((col_i < LANES + 8) & (gy < ngy - 1)) | (
        (col_i >= width - 8) & (gy > 0)
    )
    mask = jnp.where(inside_x & inside_y, 1.0, 0.0)

    for c in range(3):
        s = surf[c]
        fields[c] = (6.0 - SHIFT) * s - (up(s, 0) + down(s, 0)) - (up(s, 1) + down(s, 1))
    s0, s1, s2 = surf[0], surf[1], surf[2]
    flux = mask * 0.5 * ((up(s0, 0) - down(s0, 0)) + (up(s1, 1) - down(s1, 1)))
    fields[3] = flux
    fields[4] = 0.5 * (up(flux, 0) - down(flux, 0))
    fields[5] = 0.5 * (up(s2, 0) - down(s2, 0))
    fields[6] = 0.5 * (up(flux, 1) - down(flux, 1))
    fields[7] = 0.5 * (up(s2, 1) - down(s2, 1))
    fields[8] = mask

    z_all = nz * ngz

    def inside_z(z):
        return jnp.where((z >= 0) & (z < z_all), 1.0, 0.0).astype(F32)

    first_z = gz * nz

    def apply_first(iz, carry):
        zg = first_z + iz - 4
        dmm, dm, d0, dp, dpp = [dext[iz + j][0:1, 0:1] for j in range(5)]
        here = inside_z(zg)
        e0 = 0.5 * here * (dp - dm)
        ep = 0.5 * inside_z(zg + 1) * (dpp - d0)
        em = 0.5 * inside_z(zg - 1) * (d0 - dmm)
        k = kext[iz]
        m = fields[8] * here
        kd = k * d0 - (dm + dp)
        v1[0, iz] = m * (d0 * fields[0] + kd * surf[0]
                         - KAPPA * (d0 * fields[4] + e0 * fields[5]))
        v1[1, iz] = m * (d0 * fields[1] + kd * surf[1]
                         - KAPPA * (d0 * fields[6] + e0 * fields[7]))
        v1[2, iz] = m * (d0 * fields[2] + kd * surf[2]
                         - (0.5 * KAPPA) * ((dp - dm) * fields[3] + (ep - em) * surf[2]))
        return carry

    lax.fori_loop(0, nz + 8, apply_first, 0)

    def again(source, planes, store):
        offset = (nz - planes) // 2

        def spread_of(iz, carry):
            zg = first_z + offset + iz - 1
            a = source[0, iz + 1]
            b = source[1, iz + 1]
            w = (up(a, 0) - down(a, 0)) + (up(b, 1) - down(b, 1))
            w = w + (source[2, iz + 2] - source[2, iz])
            div[iz] = (0.5 * inside_z(zg)) * fields[8] * w
            return carry

        lax.fori_loop(0, planes + 2, spread_of, 0)

        def image_of(iz, carry):
            zg = first_z + offset + iz
            k = kext[iz + offset + 4] + (6.0 - SHIFT)
            here = div[iz + 1]
            slopes = (
                up(here, 0) - down(here, 0),
                up(here, 1) - down(here, 1),
                div[iz + 2] - div[iz],
            )
            m = inside_z(zg) * fields[8]
            for c in range(3):
                a = source[c, iz + 2]
                near = (up(a, 0) + down(a, 0)) + (up(a, 1) + down(a, 1))
                near = near + (source[c, iz + 1] + source[c, iz + 3])
                store(c, iz, m * (k * a - near - (0.5 * KAPPA) * slopes[c]))
            return carry

        lax.fori_loop(0, planes, image_of, 0)

    def store2(c, iz, value):
        v2[c, iz] = value

    def store3(c, iz, value):
        v3[c, iz] = value[HX:HX + lx, 0:LANES]

    def emit(src, out, number):
        return pltpu.make_async_copy(src, out, out_sem.at[number])

    outs = [
        emit(v1.at[:, pl.ds(4, nz), pl.ds(HX, lx), pl.ds(0, LANES)], v1_out, 0),
        emit(v2.at[:, pl.ds(2, nz), pl.ds(HX, lx), pl.ds(0, LANES)], v2_out, 1),
        emit(v3, v3_out, 2),
    ]
    outs[0].start()
    again(v1, nz + 4, store2)
    outs[1].start()
    again(v2, nz, store3)
    outs[2].start()

    def fold(a):
        return jnp.sum(a.reshape(lx // 8, 8, LANES), axis=0)

    def products(iz, acc):
        d0 = dext[iz + 6][0:1, 0:1]
        acc = list(acc)
        for c in range(3):
            a0 = d0 * surf[c, HX:HX + lx, 0:LANES]
            a1 = v1[c, iz + 4, HX:HX + lx, 0:LANES]
            a2 = v2[c, iz + 2, HX:HX + lx, 0:LANES]
            a3 = v3[c, iz]
            for i, (a, b) in enumerate(
                ((a0, a0), (a0, a1), (a1, a1), (a1, a2), (a2, a2), (a2, a3))
            ):
                acc[i] = acc[i] + fold(a * b)
        return tuple(acc)

    acc = lax.fori_loop(0, nz, products, tuple([jnp.zeros((8, LANES), F32)] * 6))
    sub8 = lax.broadcasted_iota(jnp.int32, (8, LANES), 0)
    packed = jnp.zeros((8, LANES), F32)
    for i in range(6):
        packed = jnp.where(sub8 == i, jnp.sum(acc[i], axis=0, keepdims=True), packed)
    momsend[...] = packed
    mom[flat] = packed
    reduces = []
    for t in range(1, total):
        p, device = peer_of(t)
        q = lax.rem(flat + total - t, total)
        out = copy(momsend, mom.at[flat], r_send.at[t], r_recv.at[flat], device)
        out.start()
        reduces.append((out, copy(momsend, mom.at[q], r_send.at[t], r_recv.at[q], device)))
    for _, came in reduces:
        came.wait_recv()
    added = mom[0]
    for t in range(1, total):
        added = added + mom[t]
    mu = jnp.sum(added, axis=1, keepdims=True)
    mu = [jnp.broadcast_to(mu[i:i + 1, :], (1, LANES)) for i in range(6)]

    def inner(a, b):
        out = None
        for i, p in enumerate(a):
            for j, r in enumerate(b):
                if p is None or r is None:
                    continue
                term = p * r * mu[i + j]
                out = term if out is None else out + term
        return out

    def plus(a, factor, b):
        out = []
        for p, r in zip(a, b):
            if r is None:
                out.append(p)
            elif p is None:
                out.append(factor * r)
            else:
                out.append(p + factor * r)
        return out

    one = jnp.ones((1, LANES), F32)
    x = [None] * 4
    r = [one, None, None, None]
    p = [one, None, None, None]
    rr = mu[0]
    for step in range(ITERS):
        ap = [None] + p[:3]
        ap = plus(ap, SHIFT * one, p)
        alpha = rr / inner(p, ap)
        x = plus(x, alpha, p)
        r = plus(r, -alpha, ap)
        if step + 1 < ITERS:
            new = inner(r, r)
            p = plus(r, new / rr, p)
            rr = new
    rows = x[:3] + r
    result = jnp.zeros((8, LANES), F32)
    for i, value in enumerate(rows):
        result = jnp.where(sub8 == i, value, result)
    coef_out[...] = result

    for data, note, _, _ in exchange:
        data.wait_send()
        note.wait_send()
    for there, out in sends:
        if there is None:
            out.wait_send()
        else:
            pl.when(there)(lambda out=out: out.wait_send())
    for out, _ in reduces:
        out.wait_send()
    for out in outs:
        out.wait()


def per_device(
    ngx, ngy, ngz,
    observed, predicted, coherence_mask, block_count, block_owner,
    block_matrix_choice, block_patch, look_vector, interp_weights, depth_kernel, stiffness,
):
    blocks, epochs, pixels = observed.shape
    owners = ngx * ngy
    total = owners * ngz
    cap = max(8, 2 * blocks // owners)
    nz, lx, ly = stiffness.shape
    rows_x = lx + 2 * HX
    width = 2 * LANES
    cells = PATCH_X * PATCH_Y
    meta_w = -(-owners * cap // LANES) * LANES
    packs = -(-3 * lx // 64)
    column = lax.broadcasted_iota(jnp.int32, (blocks, pixels), 1)
    valid = coherence_mask.astype(F32) * (column < block_count[:, None]).astype(F32)
    resid = (predicted - observed) * valid[:, None, :]
    partial = jnp.stack([jnp.sum(resid * resid), jnp.sum(valid)])
    coeffs = jnp.stack(
        [sum(look_vector[e, c] * resid[:, e, :] for e in range(epochs)) for c in range(3)], axis=1
    ).astype(BF16)
    coeffs = jnp.pad(coeffs, ((0, 0), (0, 5), (0, 0)))
    vmem = pl.BlockSpec(memory_space=pltpu.VMEM)
    smem = pl.BlockSpec(memory_space=pltpu.SMEM)
    hbm = pl.BlockSpec(memory_space=pl.ANY)
    dma = pltpu.SemaphoreType.DMA
    field = jax.ShapeDtypeStruct((3, nz, lx, ly), F32)

    def buf(*shape):
        return pltpu.VMEM(shape, F32)

    v1, v2, v3, surf, coef = pl.pallas_call(
        functools.partial(body, ngx, ngy, ngz, cap, epochs),
        out_shape=[field, field, field,
                   jax.ShapeDtypeStruct((3, lx, ly), F32),
                   jax.ShapeDtypeStruct((8, LANES), F32)],
        in_specs=[smem, smem, smem, vmem, vmem, vmem, vmem, vmem],
        out_specs=[hbm, hbm, hbm, vmem, vmem],
        scratch_shapes=[
            buf(blocks, 8, cells),
            buf(owners, 3 * cap, cells),
            buf(owners, 8, meta_w),
            buf(owners, 3 * cap, cells),
            buf(owners, 8, meta_w),
            buf(3, lx, ly),
            buf(2, packs, 8, LANES),
            buf(8, LANES),
            buf(2, ngz, 3, 8, LANES),
            buf(3, 2, ngz, packs, 8, LANES),
            buf(ngz, 3, lx, ly),
            buf(ngz, 8, LANES),
            buf(nz + 12, 8, LANES),
            buf(nz + 8, rows_x, width),
            buf(2, nz // 8, rows_x, LANES),
            buf(2, nz // 8, rows_x, LANES),
            buf(3, rows_x, width),
            buf(3, nz + 8, rows_x, width),
            buf(3, nz + 4, rows_x, width),
            buf(3, nz, lx, ly),
            buf(nz + 6, rows_x, width),
            buf(9, rows_x, width),
            buf(8, LANES),
            buf(total, 8, LANES),
            dma((owners,)), dma((owners,)), dma((owners,)), dma((owners,)),
            dma((4,)), dma((4,)), dma((4,)), dma((4,)),
            dma((2 * ngz + 8 * ngz,)),
            dma((2, ngz)), dma((3, 2, ngz)), dma((ngz,)), dma((ngz,)),
            dma((total,)), dma((total,)), dma((3,)),
        ],
        compiler_params=pltpu.CompilerParams(
            collective_id=0, has_side_effects=True, vmem_limit_bytes=48 * 1024 * 1024
        ),
    )(
        block_matrix_choice, depth_kernel, partial, block_owner, block_patch[:, None],
        coeffs, interp_weights, stiffness,
    )
    c = coef[:, 0]
    v0 = depth_kernel[None, :, None, None] * surf[:, None, :, :]
    adjoint_field = c[0] * v0 + c[1] * v1 + c[2] * v2
    cg_residual = c[3] * v0 + c[4] * v1 + c[5] * v2 + c[6] * v3
    return adjoint_field, cg_residual


def solution(mesh):
    spread = P(("grp", "gx", "gy", "gz"))
    in_specs = (
        P(("grp", "gx", "gy", "gz"), None, None),
        P(("grp", "gx", "gy", "gz"), None, None),
        P(("grp", "gx", "gy", "gz"), None),
        spread,
        P(("grp", "gx", "gy", "gz"), None),
        spread,
        spread,
        P(),
        P(),
        P(("grp", "gz")),
        P(("grp", "gz"), "gx", "gy"),
    )
    out_specs = (P(None, ("grp", "gz"), "gx", "gy"), P(None, ("grp", "gz"), "gx", "gy"))
    step = functools.partial(per_device, mesh.shape["gx"], mesh.shape["gy"], mesh.shape["gz"])
    return jax.shard_map(
        step, mesh=mesh, in_specs=in_specs, out_specs=out_specs, check_vma=False
    )
```

```python
import functools

import jax
import jax.numpy as jnp
from jax import lax
from jax.experimental import pallas as pl
from jax.experimental.pallas import tpu as pltpu
from jax.sharding import PartitionSpec as P

PATCH_X = 8
PATCH_Y = 16
ITERS = 3
KAPPA = 0.5
EPS = 1e-06
SHIFT = 8.0
HX = 8
LANES = 128
VMEM_ALL = 67043328
MESH = pl.DeviceIdType.MESH
F32 = jnp.float32
BF16 = jnp.bfloat16


def split_dot(one_hot, values):
    high = values.astype(BF16)
    low = (values - high.astype(F32)).astype(BF16)
    return jnp.dot(one_hot, high, preferred_element_type=F32) + jnp.dot(
        one_hot, low, preferred_element_type=F32
    )


def dot_split(values, one_hot):
    high = values.astype(BF16)
    low = (values - high.astype(F32)).astype(BF16)
    return jnp.dot(high, one_hot, preferred_element_type=F32) + jnp.dot(
        low, one_hot, preferred_element_type=F32
    )


def up(a, axis):
    return pltpu.roll(a, a.shape[axis] - 1, axis)


def down(a, axis):
    return pltpu.roll(a, 1, axis)


def lane_roll(a, amount):
    amount = amount % LANES
    return a if amount == 0 else pltpu.roll(a, amount, a.ndim - 1)


def body(
    ngx, ngy, ngz, cap, epochs,
    choice, depth, look, owner_ref, patch_ref, count_ref, mask_ref,
    observed_hbm, predicted_hbm, weights_hbm, stiff_hbm,
    v1_out, v2_out, v3_out, surf_out, coef_out,
    observed, predicted, weights, usable, coeffs, in_sem,
    sums, send, meta, recv, metarecv, part, ppk, msum, sx, sy, sc, mz,
    dext, kext, pk, pkrecv, surf, v1, v2, v3, div, fields, momsend, mom,
    a_send, a_recv, m_send, m_recv, kx_sem, ky_sem, kz_sem, dz_sem,
    h_send, sx_sem, sy_sem, sc_sem, mz_sem, r_send, r_recv, out_sem,
):
    gx = lax.axis_index("gx")
    gy = lax.axis_index("gy")
    gz = lax.axis_index("gz")
    owners = ngx * ngy
    total = owners * ngz
    me = gx * ngy + gy
    flat = me * ngz + gz
    nz, lx, ly = stiff_hbm.shape
    blocks = choice.shape[0]
    rows_x = lx + 2 * HX
    width = 2 * LANES
    places_x = lx // PATCH_X
    places_y = ly // PATCH_Y
    places = places_x * places_y
    cells = PATCH_X * PATCH_Y
    slots = owners * cap
    meta_w = meta.shape[2]

    def at(x, y, z):
        return {"gx": x, "gy": y, "gz": z}

    def peer_of(t):
        p = lax.rem(flat + t, total)
        q = p // ngz
        return p, at(q // ngy, lax.rem(q, ngy), lax.rem(p, ngz))

    barrier = pltpu.get_barrier_semaphore()

    def greet(t, carry):
        _, device = peer_of(t)
        pl.semaphore_signal(barrier, inc=1, device_id=device, device_id_type=MESH)
        return carry

    lax.fori_loop(1, total, greet, 0)

    def copy(src, dst, send_sem, recv_sem, device):
        return pltpu.make_async_remote_copy(
            src_ref=src, dst_ref=dst, send_sem=send_sem, recv_sem=recv_sem,
            device_id=device, device_id_type=MESH,
        )

    core = kext.at[pl.ds(4, nz), pl.ds(HX, lx), pl.ds(0, LANES)]
    loads = [
        pltpu.make_async_copy(src, dst, in_sem.at[i])
        for i, (src, dst) in enumerate((
            (observed_hbm, observed), (predicted_hbm, predicted),
            (stiff_hbm, core), (weights_hbm, weights),
        ))
    ]
    for load in loads:
        load.start()

    rows_i = lax.broadcasted_iota(jnp.int32, (blocks, blocks), 0)
    cols_i = lax.broadcasted_iota(jnp.int32, (blocks, blocks), 1)

    def column_of(row):
        wide = jnp.broadcast_to(row, (blocks, blocks))
        return jnp.sum(jnp.where(rows_i == cols_i, wide, 0), axis=1, keepdims=True)

    pixels = mask_ref.shape[1]
    pixel = lax.broadcasted_iota(jnp.int32, (blocks, pixels), 1)
    valid = jnp.where(pixel < column_of(count_ref[...]), mask_ref[...], 0).astype(F32)
    usable[...] = valid

    def total_of(a):
        return jnp.sum(jnp.sum(a, axis=0, keepdims=True), axis=1, keepdims=True)

    weight = total_of(valid)
    for z in range(nz):
        dext[z + 6] = jnp.full((8, LANES), depth[z], F32)
    component = lax.broadcasted_iota(jnp.int32, (8, pixels), 0)
    views = []
    for e in range(epochs):
        view = jnp.zeros((8, pixels), F32)
        for c in range(3):
            view = jnp.where(component == c, look[e, c], view)
        views.append(view)

    loads[0].wait()
    loads[1].wait()
    squares = jnp.zeros((epochs, pixels), F32)
    for b in range(blocks):
        resid = (predicted[b] - observed[b]) * jnp.broadcast_to(
            usable[b:b + 1, :], (epochs, pixels)
        )
        squares = squares + resid * resid
        seen = None
        for e in range(epochs):
            term = jnp.broadcast_to(resid[e:e + 1, :], (8, pixels)) * views[e]
            seen = term if seen is None else seen + term
        coeffs[b] = seen.astype(BF16)
    misfit = total_of(squares)

    loads[2].wait()
    pl.semaphore_wait(barrier, total - 1)

    def both_sides(position, count, axis, low_src, low_dst, high_src, high_dst, sem, fill):
        others = {"gx": gx, "gy": gy, "gz": gz}
        lower, upper = dict(others), dict(others)
        lower[axis] = position - 1
        upper[axis] = position + 1
        to_low = copy(low_src, high_dst, sem.at[0], sem.at[1], lower)
        to_high = copy(high_src, low_dst, sem.at[2], sem.at[3], upper)
        has_low = position > 0
        has_high = position < count - 1
        pl.when(has_low)(lambda: to_low.start())
        pl.when(has_high)(lambda: to_high.start())
        pl.when(jnp.logical_not(has_low))(lambda: fill(low_dst))
        pl.when(jnp.logical_not(has_high))(lambda: fill(high_dst))

        def finish():
            @pl.when(has_low)
            def _():
                to_low.wait_send()
                copy(low_src, low_dst, sem.at[2], sem.at[3], lower).wait_recv()

            @pl.when(has_high)
            def _():
                to_high.wait_send()
                copy(high_src, high_dst, sem.at[0], sem.at[1], upper).wait_recv()

        return finish

    def zero(ref):
        ref[...] = jnp.zeros(ref.shape, F32)

    finish_x = both_sides(
        gx, ngx, "gx",
        kext.at[pl.ds(4, nz), pl.ds(HX, HX), pl.ds(0, LANES)],
        kext.at[pl.ds(4, nz), pl.ds(0, HX), pl.ds(0, LANES)],
        kext.at[pl.ds(4, nz), pl.ds(lx, HX), pl.ds(0, LANES)],
        kext.at[pl.ds(4, nz), pl.ds(HX + lx, HX), pl.ds(0, LANES)],
        kx_sem, zero,
    )
    finish_d = both_sides(
        gz, ngz, "gz",
        dext.at[pl.ds(6, 6)], dext.at[pl.ds(0, 6)],
        dext.at[pl.ds(nz, 6)], dext.at[pl.ds(nz + 6, 6)],
        dz_sem, zero,
    )

    loads[3].wait()
    for b in range(blocks):
        sums[b] = jnp.dot(coeffs[b], weights[choice[b]], preferred_element_type=F32)

    owner_row = owner_ref[...]
    patch_col = column_of(patch_ref[...])
    same = column_of(owner_row) == owner_row
    rank_row = jnp.sum(jnp.where(same & (rows_i < cols_i), 1, 0), axis=0, keepdims=True)
    rank_col = jnp.sum(jnp.where(same & (cols_i < rows_i), 1, 0), axis=1, keepdims=True)
    slot_row = owner_row * cap + rank_row
    slot_ids = lax.broadcasted_iota(jnp.int32, (slots, blocks), 0)
    select = jnp.where(slot_ids == slot_row, 1.0, 0.0).astype(BF16)
    for c in range(3):
        sent = split_dot(select, sums[:, c, :])
        send[:, c * cap:(c + 1) * cap, :] = sent.reshape(owners, cap, cells)
    lane_ids = lax.broadcasted_iota(jnp.int32, (blocks, meta_w), 1)
    ranked = jnp.where(lane_ids == rank_col + me * cap, patch_col, 0).astype(F32).astype(BF16)
    owner_ids = lax.broadcasted_iota(jnp.int32, (max(8, owners), blocks), 0)
    owner_hot = jnp.where(owner_ids == owner_row, 1.0, 0.0).astype(BF16)
    patches = jnp.dot(owner_hot, ranked, preferred_element_type=F32)
    sub_ids = lax.broadcasted_iota(jnp.int32, (8, meta_w), 0)
    extras = jnp.where(sub_ids == 1, misfit, jnp.where(sub_ids == 2, weight, 0.0))
    for o in range(owners):
        line = jnp.broadcast_to(patches[o:o + 1, :], (8, meta_w))
        meta[o] = jnp.where(sub_ids == 0, line, extras)

    exchange = []
    for t in range(1, owners):
        o = lax.rem(me + t, owners)
        src = lax.rem(me + owners - t, owners)
        device = at(o // ngy, lax.rem(o, ngy), gz)
        data = copy(send.at[o], recv.at[me], a_send.at[t], a_recv.at[me], device)
        note = copy(meta.at[o], metarecv.at[me], m_send.at[t], m_recv.at[me], device)
        data.start()
        note.start()
        exchange.append((
            data, note,
            copy(send.at[o], recv.at[src], a_send.at[t], a_recv.at[src], device),
            copy(meta.at[o], metarecv.at[src], m_send.at[t], m_recv.at[src], device),
        ))

    finish_x()
    lane1 = lax.broadcasted_iota(jnp.int32, (rows_x, LANES), 1)
    for g in range(nz // 8):
        left = jnp.zeros((rows_x, LANES), F32)
        right = jnp.zeros((rows_x, LANES), F32)
        for k in range(8):
            plane = kext[4 + 8 * g + k, :, 0:LANES]
            here = (lane1 // 16) == k
            left = jnp.where(here, lane_roll(plane, 16 * k), left)
            right = jnp.where(here, lane_roll(plane, 16 * k + 16), right)
        pk[0, g] = left
        pk[1, g] = right
    finish_y = both_sides(
        gy, ngy, "gy", pk.at[0], pkrecv.at[0], pk.at[1], pkrecv.at[1], ky_sem, zero
    )
    recv[me] = send[me]
    metarecv[me] = meta[me]
    for data, note, data_in, note_in in exchange:
        data_in.wait_recv()
        note_in.wait_recv()

    notes = metarecv[0]
    for s in range(1, owners):
        notes = notes + metarecv[s]
    patch_row = notes[0:1, 0:slots]
    place_ids = lax.broadcasted_iota(jnp.int32, (places, slots), 0).astype(F32)
    place_hot = jnp.where(place_ids == patch_row, 1.0, 0.0).astype(BF16)
    msum[...] = notes[:, 0:LANES]
    cell_i = lax.broadcasted_iota(jnp.int32, (cells, PATCH_X * LANES), 0)
    lane_i = lax.broadcasted_iota(jnp.int32, (cells, PATCH_X * LANES), 1)
    spread = jnp.where(
        cell_i == (lane_i // LANES) * PATCH_Y + lane_i % PATCH_Y, 1.0, 0.0
    ).astype(BF16)
    wide_lane = lax.broadcasted_iota(jnp.int32, (places, PATCH_X * LANES), 1)
    wide_row = lax.broadcasted_iota(jnp.int32, (places, PATCH_X * LANES), 0)
    own_place = (wide_lane % LANES) // PATCH_Y == wide_row % places_y
    for c in range(3):
        arrived = recv[:, c * cap:(c + 1) * cap, :].reshape(slots, cells)
        placed = split_dot(place_hot, arrived)
        expanded = jnp.where(own_place, dot_split(placed, spread), 0.0)
        lines = jnp.sum(expanded.reshape(places_x, places_y, PATCH_X * LANES), axis=1)
        for i in range(PATCH_X):
            for px in range(places_x):
                row = px * PATCH_X + i
                part[c, row:row + 1, :] = lines[px:px + 1, i * LANES:(i + 1) * LANES]

    lane8 = lax.broadcasted_iota(jnp.int32, (8, LANES), 1)
    groups = lx // 8
    packs = ppk.shape[1]
    left = [jnp.zeros((8, LANES), F32)] * packs
    right = [jnp.zeros((8, LANES), F32)] * packs
    for c in range(3):
        for r in range(groups):
            k = c * groups + r
            q, kk = k // 8, k % 8
            tile = part[c, r * 8:(r + 1) * 8, :]
            here = (lane8 // 16) == kk
            left[q] = jnp.where(here, lane_roll(tile, 16 * kk), left[q])
            right[q] = jnp.where(here, lane_roll(tile, 16 * kk + 16), right[q])
    for q in range(packs):
        ppk[0, q] = left[q]
        ppk[1, q] = right[q]

    sends, receives = [], []
    number = 0
    for t in range(1, ngz):
        z = lax.rem(gz + t, ngz)
        for src, dst, sem in ((part, sc, sc_sem), (msum, mz, mz_sem)):
            out = copy(src, dst.at[gz], h_send.at[number], sem.at[gz], at(gx, gy, z))
            out.start()
            sends.append((None, out))
            receives.append((None, copy(src, dst.at[z], h_send.at[number], sem.at[z], at(gx, gy, z))))
            number += 1
    for dx in (-1, 0, 1):
        for dy in (-1, 0, 1):
            if dx == 0 and dy == 0:
                continue
            nx, ny = gx + dx, gy + dy
            there = (nx >= 0) & (nx < ngx) & (ny >= 0) & (ny < ngy)
            for z in range(ngz):
                device = at(nx, ny, z)
                if dy == 0:
                    src = part.at[:, pl.ds(lx - 8 if dx > 0 else 0, 8), :]
                    side_out, side_in = (0, 1) if dx > 0 else (1, 0)
                    out = copy(src, sx.at[side_out, gz], h_send.at[number],
                               sx_sem.at[side_out, gz], device)
                    came = copy(src, sx.at[side_in, z], h_send.at[number],
                                sx_sem.at[side_in, z], device)
                    hole = sx.at[side_in, z]
                else:
                    src = ppk.at[1 if dy > 0 else 0]
                    side_out, side_in = (0, 1) if dy > 0 else (1, 0)
                    out = copy(src, sy.at[1 - dx, side_out, gz], h_send.at[number],
                               sy_sem.at[1 - dx, side_out, gz], device)
                    came = copy(src, sy.at[1 + dx, side_in, z], h_send.at[number],
                                sy_sem.at[1 + dx, side_in, z], device)
                    hole = sy.at[1 + dx, side_in, z]
                pl.when(there)(lambda out=out: out.start())
                pl.when(jnp.logical_not(there))(lambda hole=hole: zero(hole))
                sends.append((there, out))
                receives.append((there, came))
                number += 1
    sc[gz] = part[...]
    mz[gz] = msum[...]
    finish_d()
    finish_y()
    for g in range(nz // 8):
        from_left = pkrecv[0, g]
        from_right = pkrecv[1, g]
        for k in range(8):
            kext[4 + 8 * g + k, :, LANES:width] = jnp.where(
                lane1 < 64, lane_roll(from_right, -16 * k), lane_roll(from_left, 112 - 16 * k)
            )
    finish_z = both_sides(
        gz, ngz, "gz",
        kext.at[pl.ds(4, 4)], kext.at[pl.ds(0, 4)],
        kext.at[pl.ds(nz, 4)], kext.at[pl.ds(nz + 4, 4)],
        kz_sem, zero,
    )

    for there, came in receives:
        if there is None:
            came.wait_recv()
        else:
            pl.when(there)(lambda came=came: came.wait_recv())

    tot = mz[0]
    for z in range(1, ngz):
        tot = tot + mz[z]
    scale = lax.rsqrt(tot[1:2, :] / (epochs * tot[2:3, :]) + EPS)

    def over_gz(ref, *index):
        value = ref[index + (0,)]
        for z in range(1, ngz):
            value = value + ref[index + (z,)]
        return value

    centre = over_gz(sc) * scale
    surf[:, HX:HX + lx, 0:LANES] = centre
    surf_out[...] = centre
    surf[:, 0:HX, 0:LANES] = over_gz(sx, 0) * scale
    surf[:, HX + lx:, 0:LANES] = over_gz(sx, 1) * scale
    edge_lane = (lane8 < 8) | (lane8 >= LANES - 8)
    for d in range(3):
        from_left = over_gz(sy, d, 0)
        from_right = over_gz(sy, d, 1)
        for c in range(3):
            for r in ((groups - 1,), range(groups), (0,))[d]:
                k = c * groups + r
                q, kk = k // 8, k % 8
                tile = jnp.where(
                    lane8 < 64, lane_roll(from_right[q], -16 * kk),
                    lane_roll(from_left[q], 112 - 16 * kk),
                )
                row = (0, HX + r * 8, HX + lx)[d]
                surf[c, row:row + 8, LANES:width] = jnp.where(edge_lane, tile * scale, 0.0)

    row_i = lax.broadcasted_iota(jnp.int32, (rows_x, width), 0)
    col_i = lax.broadcasted_iota(jnp.int32, (rows_x, width), 1)
    inside_x = ((row_i >= HX) | (gx > 0)) & ((row_i < HX + lx) | (gx < ngx - 1))
    inside_y = (col_i < LANES) | ((col_i < LANES + 8) & (gy < ngy - 1)) | (
        (col_i >= width - 8) & (gy > 0)
    )
    mask = jnp.where(inside_x & inside_y, 1.0, 0.0)

    for c in range(3):
        s = surf[c]
        fields[c] = (6.0 - SHIFT) * s - (up(s, 0) + down(s, 0)) - (up(s, 1) + down(s, 1))
    s0, s1, s2 = surf[0], surf[1], surf[2]
    flux = mask * 0.5 * ((up(s0, 0) - down(s0, 0)) + (up(s1, 1) - down(s1, 1)))
    fields[3] = flux
    fields[4] = 0.5 * (up(flux, 0) - down(flux, 0))
    fields[5] = 0.5 * (up(s2, 0) - down(s2, 0))
    fields[6] = 0.5 * (up(flux, 1) - down(flux, 1))
    fields[7] = 0.5 * (up(s2, 1) - down(s2, 1))
    fields[8] = mask

    z_all = nz * ngz

    def inside_z(z):
        return jnp.where((z >= 0) & (z < z_all), 1.0, 0.0).astype(F32)

    first_z = gz * nz

    def apply_first(iz, carry):
        zg = first_z + iz - 4
        dmm, dm, d0, dp, dpp = [dext[iz + j][0:1, 0:1] for j in range(5)]
        here = inside_z(zg)
        e0 = 0.5 * here * (dp - dm)
        ep = 0.5 * inside_z(zg + 1) * (dpp - d0)
        em = 0.5 * inside_z(zg - 1) * (d0 - dmm)
        k = kext[iz]
        m = fields[8] * here
        kd = k * d0 - (dm + dp)
        v1[0, iz] = m * (d0 * fields[0] + kd * surf[0]
                         - KAPPA * (d0 * fields[4] + e0 * fields[5]))
        v1[1, iz] = m * (d0 * fields[1] + kd * surf[1]
                         - KAPPA * (d0 * fields[6] + e0 * fields[7]))
        v1[2, iz] = m * (d0 * fields[2] + kd * surf[2]
                         - (0.5 * KAPPA) * ((dp - dm) * fields[3] + (ep - em) * surf[2]))
        return carry

    finish_z()
    lax.fori_loop(0, nz + 8, apply_first, 0)

    def again(source, planes, store):
        offset = (nz - planes) // 2

        def spread_of(iz, carry):
            zg = first_z + offset + iz - 1
            a = source[0, iz + 1]
            b = source[1, iz + 1]
            w = (up(a, 0) - down(a, 0)) + (up(b, 1) - down(b, 1))
            w = w + (source[2, iz + 2] - source[2, iz])
            div[iz] = (0.5 * inside_z(zg)) * fields[8] * w
            return carry

        lax.fori_loop(0, planes + 2, spread_of, 0)

        def image_of(iz, carry):
            zg = first_z + offset + iz
            k = kext[iz + offset + 4] + (6.0 - SHIFT)
            here = div[iz + 1]
            slopes = (
                up(here, 0) - down(here, 0),
                up(here, 1) - down(here, 1),
                div[iz + 2] - div[iz],
            )
            m = inside_z(zg) * fields[8]
            for c in range(3):
                a = source[c, iz + 2]
                near = (up(a, 0) + down(a, 0)) + (up(a, 1) + down(a, 1))
                near = near + (source[c, iz + 1] + source[c, iz + 3])
                store(c, iz, m * (k * a - near - (0.5 * KAPPA) * slopes[c]))
            return carry

        lax.fori_loop(0, planes, image_of, 0)

    def store2(c, iz, value):
        v2[c, iz] = value

    def store3(c, iz, value):
        v3[c, iz] = value[HX:HX + lx, 0:LANES]

    outs = [
        pltpu.make_async_copy(src, dst, out_sem.at[i])
        for i, (src, dst) in enumerate((
            (v1.at[:, pl.ds(4, nz), pl.ds(HX, lx), pl.ds(0, LANES)], v1_out),
            (v2.at[:, pl.ds(2, nz), pl.ds(HX, lx), pl.ds(0, LANES)], v2_out),
            (v3, v3_out),
        ))
    ]
    outs[0].start()
    again(v1, nz + 4, store2)
    outs[1].start()
    again(v2, nz, store3)
    outs[2].start()

    def fold(a):
        return jnp.sum(a.reshape(lx // 8, 8, LANES), axis=0)

    def products(iz, acc):
        d0 = dext[iz + 6][0:1, 0:1]
        acc = list(acc)
        for c in range(3):
            a0 = d0 * surf[c, HX:HX + lx, 0:LANES]
            a1 = v1[c, iz + 4, HX:HX + lx, 0:LANES]
            a2 = v2[c, iz + 2, HX:HX + lx, 0:LANES]
            a3 = v3[c, iz]
            for i, (a, b) in enumerate(
                ((a0, a0), (a0, a1), (a1, a1), (a1, a2), (a2, a2), (a2, a3))
            ):
                acc[i] = acc[i] + fold(a * b)
        return tuple(acc)

    acc = lax.fori_loop(0, nz, products, tuple([jnp.zeros((8, LANES), F32)] * 6))
    sub8 = lax.broadcasted_iota(jnp.int32, (8, LANES), 0)
    packed = jnp.zeros((8, LANES), F32)
    for i in range(6):
        packed = jnp.where(sub8 == i, jnp.sum(acc[i], axis=0, keepdims=True), packed)
    momsend[...] = packed
    mom[flat] = packed
    reduces = []
    for t in range(1, total):
        p, device = peer_of(t)
        q = lax.rem(flat + total - t, total)
        out = copy(momsend, mom.at[flat], r_send.at[t], r_recv.at[flat], device)
        out.start()
        reduces.append((out, copy(momsend, mom.at[q], r_send.at[t], r_recv.at[q], device)))
    for _, came in reduces:
        came.wait_recv()
    added = mom[0]
    for t in range(1, total):
        added = added + mom[t]
    mu = jnp.sum(added, axis=1, keepdims=True)
    mu = [jnp.broadcast_to(mu[i:i + 1, :], (1, LANES)) for i in range(6)]

    def inner(a, b):
        out = None
        for i, p in enumerate(a):
            for j, r in enumerate(b):
                if p is None or r is None:
                    continue
                term = p * r * mu[i + j]
                out = term if out is None else out + term
        return out

    def plus(a, factor, b):
        out = []
        for p, r in zip(a, b):
            if r is None:
                out.append(p)
            elif p is None:
                out.append(factor * r)
            else:
                out.append(p + factor * r)
        return out

    one = jnp.ones((1, LANES), F32)
    x = [None] * 4
    r = [one, None, None, None]
    p = [one, None, None, None]
    rr = mu[0]
    for step in range(ITERS):
        ap = [None] + p[:3]
        ap = plus(ap, SHIFT * one, p)
        alpha = rr / inner(p, ap)
        x = plus(x, alpha, p)
        r = plus(r, -alpha, ap)
        if step + 1 < ITERS:
            new = inner(r, r)
            p = plus(r, new / rr, p)
            rr = new
    rows = x[:3] + r
    result = jnp.zeros((8, LANES), F32)
    for i, value in enumerate(rows):
        result = jnp.where(sub8 == i, value, result)
    coef_out[...] = result

    for data, note, _, _ in exchange:
        data.wait_send()
        note.wait_send()
    for there, out in sends:
        if there is None:
            out.wait_send()
        else:
            pl.when(there)(lambda out=out: out.wait_send())
    for out, _ in reduces:
        out.wait_send()
    for out in outs:
        out.wait()

def combine(
    depth, coef, surf, v1_in, v2_in, v3_in, field_out, resid_out,
    v1, v2, v3, field, resid, in_sem, sem,
):
    nz = v1.shape[1]
    chunk = 4 if nz % 4 == 0 else 1
    arriving = []
    for start in range(0, nz, chunk):
        part = pl.ds(start, chunk)
        for i, (src, dst) in enumerate(((v1_in, v1), (v2_in, v2), (v3_in, v3))):
            load = pltpu.make_async_copy(
                src.at[:, part], dst.at[:, part], in_sem.at[i, start // chunk]
            )
            load.start()
            arriving.append(load)
    factors = [coef[i:i + 1, :] for i in range(7)]
    copies = []
    for start in range(0, nz, chunk):
        for load in arriving[3 * (start // chunk):3 * (start // chunk) + 3]:
            load.wait()
        for z in range(start, start + chunk):
            for c in range(3):
                a0 = depth[z] * surf[c]
                a1, a2 = v1[c, z], v2[c, z]
                field[c, z] = factors[0] * a0 + factors[1] * a1 + factors[2] * a2
                resid[c, z] = (factors[3] * a0 + factors[4] * a1) + (
                    factors[5] * a2 + factors[6] * v3[c, z]
                )
        part = pl.ds(start, chunk)
        for i, (src, dst) in enumerate(((field, field_out), (resid, resid_out))):
            out = pltpu.make_async_copy(
                src.at[:, part], dst.at[:, part], sem.at[i, start // chunk]
            )
            out.start()
            copies.append(out)
    for out in copies:
        out.wait()


def per_device(
    ngx, ngy, ngz,
    observed, predicted, coherence_mask, block_count, block_owner,
    block_matrix_choice, block_patch, look_vector, interp_weights, depth_kernel, stiffness,
):
    blocks, epochs, pixels = observed.shape
    owners = ngx * ngy
    total = owners * ngz
    cap = max(8, 2 * blocks // owners)
    nz, lx, ly = stiffness.shape
    rows_x = lx + 2 * HX
    width = 2 * LANES
    cells = PATCH_X * PATCH_Y
    meta_w = -(-owners * cap // LANES) * LANES
    packs = -(-3 * lx // 64)
    vmem = pl.BlockSpec(memory_space=pltpu.VMEM)
    smem = pl.BlockSpec(memory_space=pltpu.SMEM)
    hbm = pl.BlockSpec(memory_space=pltpu.HBM)
    dma = pltpu.SemaphoreType.DMA
    field = jax.ShapeDtypeStruct((3, nz, lx, ly), F32)

    def buf(*shape):
        return pltpu.VMEM(shape, F32)

    v1, v2, v3, surf, coef = pl.pallas_call(
        functools.partial(body, ngx, ngy, ngz, cap, epochs),
        out_shape=[field, field, field,
                   jax.ShapeDtypeStruct((3, lx, ly), F32),
                   jax.ShapeDtypeStruct((8, LANES), F32)],
        in_specs=[smem, smem, smem, vmem, vmem, vmem, vmem, hbm, hbm, hbm, hbm],
        out_specs=[hbm, hbm, hbm, vmem, vmem],
        scratch_shapes=[
            buf(blocks, epochs, pixels),
            buf(blocks, epochs, pixels),
            pltpu.VMEM(interp_weights.shape, BF16),
            buf(blocks, pixels),
            pltpu.VMEM((blocks, 8, pixels), BF16),
            dma((4,)),
            buf(blocks, 8, cells),
            buf(owners, 3 * cap, cells),
            buf(owners, 8, meta_w),
            buf(owners, 3 * cap, cells),
            buf(owners, 8, meta_w),
            buf(3, lx, ly),
            buf(2, packs, 8, LANES),
            buf(8, LANES),
            buf(2, ngz, 3, 8, LANES),
            buf(3, 2, ngz, packs, 8, LANES),
            buf(ngz, 3, lx, ly),
            buf(ngz, 8, LANES),
            buf(nz + 12, 8, LANES),
            buf(nz + 8, rows_x, width),
            buf(2, nz // 8, rows_x, LANES),
            buf(2, nz // 8, rows_x, LANES),
            buf(3, rows_x, width),
            buf(3, nz + 8, rows_x, width),
            buf(3, nz + 4, rows_x, width),
            buf(3, nz, lx, ly),
            buf(nz + 6, rows_x, width),
            buf(9, rows_x, width),
            buf(8, LANES),
            buf(total, 8, LANES),
            dma((owners,)), dma((owners,)), dma((owners,)), dma((owners,)),
            dma((4,)), dma((4,)), dma((4,)), dma((4,)),
            dma((2 * ngz + 8 * ngz,)),
            dma((2, ngz)), dma((3, 2, ngz)), dma((ngz,)), dma((ngz,)),
            dma((total,)), dma((total,)), dma((3,)),
        ],
        compiler_params=pltpu.CompilerParams(
            collective_id=0, has_side_effects=True, vmem_limit_bytes=VMEM_ALL
        ),
    )(
        block_matrix_choice, depth_kernel, look_vector, block_owner.reshape(1, blocks),
        block_patch[None, :], block_count[None, :], coherence_mask,
        observed, predicted, interp_weights, stiffness,
    )
    return pl.pallas_call(
        combine,
        out_shape=[field, field],
        in_specs=[smem, vmem, vmem, hbm, hbm, hbm],
        out_specs=[hbm, hbm],
        scratch_shapes=[buf(3, nz, lx, ly)] * 5 + [dma((3, nz)), dma((2, nz))],
        compiler_params=pltpu.CompilerParams(vmem_limit_bytes=VMEM_ALL),
    )(depth_kernel, coef, surf, v1, v2, v3)


def solution(mesh):
    spread = P(("grp", "gx", "gy", "gz"))
    in_specs = (
        P(("grp", "gx", "gy", "gz"), None, None),
        P(("grp", "gx", "gy", "gz"), None, None),
        P(("grp", "gx", "gy", "gz"), None),
        spread,
        P(("grp", "gx", "gy", "gz"), None),
        spread,
        spread,
        P(),
        P(),
        P(("grp", "gz")),
        P(("grp", "gz"), "gx", "gy"),
    )
    out_specs = (P(None, ("grp", "gz"), "gx", "gy"), P(None, ("grp", "gz"), "gx", "gy"))
    step = functools.partial(per_device, mesh.shape["gx"], mesh.shape["gy"], mesh.shape["gz"])
    return jax.shard_map(
        step, mesh=mesh, in_specs=in_specs, out_specs=out_specs, check_vma=False
    )
```

```python
import functools

import jax
import jax.numpy as jnp
from jax import lax
from jax.experimental import pallas as pl
from jax.experimental.pallas import tpu as pltpu
from jax.sharding import PartitionSpec as P

PATCH_X = 8
PATCH_Y = 16
ITERS = 3
KAPPA = 0.5
EPS = 1e-06
SHIFT = 8.0
HX = 8
LANES = 128
VMEM_ALL = 67043328
MESH = pl.DeviceIdType.MESH
F32 = jnp.float32
BF16 = jnp.bfloat16


def split_dot(one_hot, values):
    high = values.astype(BF16)
    low = (values - high.astype(F32)).astype(BF16)
    return jnp.dot(one_hot, high, preferred_element_type=F32) + jnp.dot(
        one_hot, low, preferred_element_type=F32
    )


def dot_split(values, one_hot):
    high = values.astype(BF16)
    low = (values - high.astype(F32)).astype(BF16)
    return jnp.dot(high, one_hot, preferred_element_type=F32) + jnp.dot(
        low, one_hot, preferred_element_type=F32
    )


def up(a, axis):
    return pltpu.roll(a, a.shape[axis] - 1, axis)


def down(a, axis):
    return pltpu.roll(a, 1, axis)


def lane_roll(a, amount):
    amount = amount % LANES
    return a if amount == 0 else pltpu.roll(a, amount, a.ndim - 1)


def body(
    ngx, ngy, ngz, cap, epochs,
    choice, depth, look, owner_ref, patch_ref, count_ref, mask_ref,
    observed_hbm, predicted_hbm, weights_hbm, stiff_hbm,
    v1_out, v2_out, v3_out, surf_out, coef_out,
    observed, predicted, weights, usable, coeffs, in_sem,
    sums, send, meta, recv, metarecv, part, ppk, msum, sx, sy, sc, mz,
    dext, kext, pk, pkrecv, surf, v1, v2, v3, div, fields, momsend, mom,
    a_send, a_recv, m_send, m_recv, kx_sem, ky_sem, kz_sem, dz_sem,
    h_send, sx_sem, sy_sem, sc_sem, mz_sem, r_send, r_recv, out_sem,
):
    gx = lax.axis_index("gx")
    gy = lax.axis_index("gy")
    gz = lax.axis_index("gz")
    owners = ngx * ngy
    total = owners * ngz
    me = gx * ngy + gy
    flat = me * ngz + gz
    nz, lx, ly = stiff_hbm.shape
    blocks = choice.shape[0]
    rows_x = lx + 2 * HX
    width = 2 * LANES
    places_x = lx // PATCH_X
    places_y = ly // PATCH_Y
    places = places_x * places_y
    cells = PATCH_X * PATCH_Y
    slots = owners * cap
    meta_w = meta.shape[2]

    def at(x, y, z):
        return {"gx": x, "gy": y, "gz": z}

    def peer_of(t):
        p = lax.rem(flat + t, total)
        q = p // ngz
        return p, at(q // ngy, lax.rem(q, ngy), lax.rem(p, ngz))

    barrier = pltpu.get_barrier_semaphore()

    def greet(t, carry):
        _, device = peer_of(t)
        pl.semaphore_signal(barrier, inc=1, device_id=device, device_id_type=MESH)
        return carry

    lax.fori_loop(1, total, greet, 0)

    def copy(src, dst, send_sem, recv_sem, device):
        return pltpu.make_async_remote_copy(
            src_ref=src, dst_ref=dst, send_sem=send_sem, recv_sem=recv_sem,
            device_id=device, device_id_type=MESH,
        )

    core = kext.at[pl.ds(4, nz), pl.ds(HX, lx), pl.ds(0, LANES)]
    loads = [
        pltpu.make_async_copy(src, dst, in_sem.at[i])
        for i, (src, dst) in enumerate((
            (observed_hbm, observed), (predicted_hbm, predicted),
            (stiff_hbm, core), (weights_hbm, weights),
        ))
    ]
    for load in loads:
        load.start()

    rows_i = lax.broadcasted_iota(jnp.int32, (blocks, blocks), 0)
    cols_i = lax.broadcasted_iota(jnp.int32, (blocks, blocks), 1)

    def column_of(row):
        wide = jnp.broadcast_to(row, (blocks, blocks))
        return jnp.sum(jnp.where(rows_i == cols_i, wide, 0), axis=1, keepdims=True)

    pixels = mask_ref.shape[1]
    pixel = lax.broadcasted_iota(jnp.int32, (blocks, pixels), 1)
    valid = jnp.where(pixel < column_of(count_ref[...]), mask_ref[...], 0).astype(F32)
    usable[...] = valid

    def total_of(a):
        return jnp.sum(jnp.sum(a, axis=0, keepdims=True), axis=1, keepdims=True)

    weight = total_of(valid)
    for z in range(nz):
        dext[z + 6] = jnp.full((8, LANES), depth[z], F32)
    component = lax.broadcasted_iota(jnp.int32, (8, pixels), 0)
    views = []
    for e in range(epochs):
        view = jnp.zeros((8, pixels), F32)
        for c in range(3):
            view = jnp.where(component == c, look[e, c], view)
        views.append(view)

    loads[0].wait()
    loads[1].wait()
    squares = jnp.zeros((epochs, pixels), F32)
    for b in range(blocks):
        resid = (predicted[b] - observed[b]) * jnp.broadcast_to(
            usable[b:b + 1, :], (epochs, pixels)
        )
        squares = squares + resid * resid
        seen = None
        for e in range(epochs):
            term = jnp.broadcast_to(resid[e:e + 1, :], (8, pixels)) * views[e]
            seen = term if seen is None else seen + term
        coeffs[b] = seen.astype(BF16)
    misfit = total_of(squares)

    loads[2].wait()
    pl.semaphore_wait(barrier, total - 1)

    def both_sides(position, count, axis, low_src, low_dst, high_src, high_dst, sem, fill):
        others = {"gx": gx, "gy": gy, "gz": gz}
        lower, upper = dict(others), dict(others)
        lower[axis] = position - 1
        upper[axis] = position + 1
        to_low = copy(low_src, high_dst, sem.at[0], sem.at[1], lower)
        to_high = copy(high_src, low_dst, sem.at[2], sem.at[3], upper)
        has_low = position > 0
        has_high = position < count - 1
        pl.when(has_low)(lambda: to_low.start())
        pl.when(has_high)(lambda: to_high.start())
        pl.when(jnp.logical_not(has_low))(lambda: fill(low_dst))
        pl.when(jnp.logical_not(has_high))(lambda: fill(high_dst))

        def finish():
            @pl.when(has_low)
            def _():
                to_low.wait_send()
                copy(low_src, low_dst, sem.at[2], sem.at[3], lower).wait_recv()

            @pl.when(has_high)
            def _():
                to_high.wait_send()
                copy(high_src, high_dst, sem.at[0], sem.at[1], upper).wait_recv()

        return finish

    def zero(ref):
        ref[...] = jnp.zeros(ref.shape, F32)

    finish_x = both_sides(
        gx, ngx, "gx",
        kext.at[pl.ds(4, nz), pl.ds(HX, HX), pl.ds(0, LANES)],
        kext.at[pl.ds(4, nz), pl.ds(0, HX), pl.ds(0, LANES)],
        kext.at[pl.ds(4, nz), pl.ds(lx, HX), pl.ds(0, LANES)],
        kext.at[pl.ds(4, nz), pl.ds(HX + lx, HX), pl.ds(0, LANES)],
        kx_sem, zero,
    )
    finish_d = both_sides(
        gz, ngz, "gz",
        dext.at[pl.ds(6, 6)], dext.at[pl.ds(0, 6)],
        dext.at[pl.ds(nz, 6)], dext.at[pl.ds(nz + 6, 6)],
        dz_sem, zero,
    )

    loads[3].wait()
    for b in range(blocks):
        sums[b] = jnp.dot(coeffs[b], weights[choice[b]], preferred_element_type=F32)

    owner_row = owner_ref[...]
    patch_col = column_of(patch_ref[...])
    same = column_of(owner_row) == owner_row
    rank_row = jnp.sum(jnp.where(same & (rows_i < cols_i), 1, 0), axis=0, keepdims=True)
    rank_col = jnp.sum(jnp.where(same & (cols_i < rows_i), 1, 0), axis=1, keepdims=True)
    slot_row = owner_row * cap + rank_row
    slot_ids = lax.broadcasted_iota(jnp.int32, (slots, blocks), 0)
    select = jnp.where(slot_ids == slot_row, 1.0, 0.0).astype(BF16)
    for c in range(3):
        sent = split_dot(select, sums[:, c, :])
        send[:, c * cap:(c + 1) * cap, :] = sent.reshape(owners, cap, cells)
    lane_ids = lax.broadcasted_iota(jnp.int32, (blocks, meta_w), 1)
    ranked = jnp.where(lane_ids == rank_col + me * cap, patch_col, 0).astype(F32).astype(BF16)
    owner_ids = lax.broadcasted_iota(jnp.int32, (max(8, owners), blocks), 0)
    owner_hot = jnp.where(owner_ids == owner_row, 1.0, 0.0).astype(BF16)
    patches = jnp.dot(owner_hot, ranked, preferred_element_type=F32)
    sub_ids = lax.broadcasted_iota(jnp.int32, (8, meta_w), 0)
    extras = jnp.where(sub_ids == 1, misfit, jnp.where(sub_ids == 2, weight, 0.0))
    for o in range(owners):
        line = jnp.broadcast_to(patches[o:o + 1, :], (8, meta_w))
        meta[o] = jnp.where(sub_ids == 0, line, extras)

    exchange = []
    for t in range(1, owners):
        o = lax.rem(me + t, owners)
        src = lax.rem(me + owners - t, owners)
        device = at(o // ngy, lax.rem(o, ngy), gz)
        data = copy(send.at[o], recv.at[me], a_send.at[t], a_recv.at[me], device)
        note = copy(meta.at[o], metarecv.at[me], m_send.at[t], m_recv.at[me], device)
        data.start()
        note.start()
        exchange.append((
            data, note,
            copy(send.at[o], recv.at[src], a_send.at[t], a_recv.at[src], device),
            copy(meta.at[o], metarecv.at[src], m_send.at[t], m_recv.at[src], device),
        ))

    finish_x()
    lane1 = lax.broadcasted_iota(jnp.int32, (rows_x, LANES), 1)
    for g in range(nz // 8):
        left = jnp.zeros((rows_x, LANES), F32)
        right = jnp.zeros((rows_x, LANES), F32)
        for k in range(8):
            plane = kext[4 + 8 * g + k, :, 0:LANES]
            here = (lane1 // 16) == k
            left = jnp.where(here, lane_roll(plane, 16 * k), left)
            right = jnp.where(here, lane_roll(plane, 16 * k + 16), right)
        pk[0, g] = left
        pk[1, g] = right
    finish_y = both_sides(
        gy, ngy, "gy", pk.at[0], pkrecv.at[0], pk.at[1], pkrecv.at[1], ky_sem, zero
    )
    recv[me] = send[me]
    metarecv[me] = meta[me]
    for data, note, data_in, note_in in exchange:
        data_in.wait_recv()
        note_in.wait_recv()

    notes = metarecv[0]
    for s in range(1, owners):
        notes = notes + metarecv[s]
    patch_row = notes[0:1, 0:slots]
    place_ids = lax.broadcasted_iota(jnp.int32, (places, slots), 0).astype(F32)
    place_hot = jnp.where(place_ids == patch_row, 1.0, 0.0).astype(BF16)
    msum[...] = notes[:, 0:LANES]
    cell_i = lax.broadcasted_iota(jnp.int32, (cells, PATCH_X * LANES), 0)
    lane_i = lax.broadcasted_iota(jnp.int32, (cells, PATCH_X * LANES), 1)
    spread = jnp.where(
        cell_i == (lane_i // LANES) * PATCH_Y + lane_i % PATCH_Y, 1.0, 0.0
    ).astype(BF16)
    wide_lane = lax.broadcasted_iota(jnp.int32, (places, PATCH_X * LANES), 1)
    wide_row = lax.broadcasted_iota(jnp.int32, (places, PATCH_X * LANES), 0)
    own_place = (wide_lane % LANES) // PATCH_Y == wide_row % places_y
    for c in range(3):
        arrived = recv[:, c * cap:(c + 1) * cap, :].reshape(slots, cells)
        placed = split_dot(place_hot, arrived)
        expanded = jnp.where(own_place, dot_split(placed, spread), 0.0)
        lines = jnp.sum(expanded.reshape(places_x, places_y, PATCH_X * LANES), axis=1)
        for i in range(PATCH_X):
            for px in range(places_x):
                row = px * PATCH_X + i
                part[c, row:row + 1, :] = lines[px:px + 1, i * LANES:(i + 1) * LANES]

    lane8 = lax.broadcasted_iota(jnp.int32, (8, LANES), 1)
    groups = lx // 8
    packs = ppk.shape[1]
    left = [jnp.zeros((8, LANES), F32)] * packs
    right = [jnp.zeros((8, LANES), F32)] * packs
    for c in range(3):
        for r in range(groups):
            k = c * groups + r
            q, kk = k // 8, k % 8
            tile = part[c, r * 8:(r + 1) * 8, :]
            here = (lane8 // 16) == kk
            left[q] = jnp.where(here, lane_roll(tile, 16 * kk), left[q])
            right[q] = jnp.where(here, lane_roll(tile, 16 * kk + 16), right[q])
    for q in range(packs):
        ppk[0, q] = left[q]
        ppk[1, q] = right[q]

    sends, receives = [], []
    number = 0
    for t in range(1, ngz):
        z = lax.rem(gz + t, ngz)
        for src, dst, sem in ((part, sc, sc_sem), (msum, mz, mz_sem)):
            out = copy(src, dst.at[gz], h_send.at[number], sem.at[gz], at(gx, gy, z))
            out.start()
            sends.append((None, out))
            receives.append((None, copy(src, dst.at[z], h_send.at[number], sem.at[z], at(gx, gy, z))))
            number += 1
    for dx in (-1, 0, 1):
        for dy in (-1, 0, 1):
            if dx == 0 and dy == 0:
                continue
            nx, ny = gx + dx, gy + dy
            there = (nx >= 0) & (nx < ngx) & (ny >= 0) & (ny < ngy)
            for z in range(ngz):
                device = at(nx, ny, z)
                if dy == 0:
                    src = part.at[:, pl.ds(lx - 8 if dx > 0 else 0, 8), :]
                    side_out, side_in = (0, 1) if dx > 0 else (1, 0)
                    out = copy(src, sx.at[side_out, gz], h_send.at[number],
                               sx_sem.at[side_out, gz], device)
                    came = copy(src, sx.at[side_in, z], h_send.at[number],
                                sx_sem.at[side_in, z], device)
                    hole = sx.at[side_in, z]
                else:
                    src = ppk.at[1 if dy > 0 else 0]
                    side_out, side_in = (0, 1) if dy > 0 else (1, 0)
                    out = copy(src, sy.at[1 - dx, side_out, gz], h_send.at[number],
                               sy_sem.at[1 - dx, side_out, gz], device)
                    came = copy(src, sy.at[1 + dx, side_in, z], h_send.at[number],
                                sy_sem.at[1 + dx, side_in, z], device)
                    hole = sy.at[1 + dx, side_in, z]
                pl.when(there)(lambda out=out: out.start())
                pl.when(jnp.logical_not(there))(lambda hole=hole: zero(hole))
                sends.append((there, out))
                receives.append((there, came))
                number += 1
    sc[gz] = part[...]
    mz[gz] = msum[...]
    finish_d()
    finish_y()
    for g in range(nz // 8):
        from_left = pkrecv[0, g]
        from_right = pkrecv[1, g]
        for k in range(8):
            kext[4 + 8 * g + k, :, LANES:width] = jnp.where(
                lane1 < 64, lane_roll(from_right, -16 * k), lane_roll(from_left, 112 - 16 * k)
            )
    finish_z = both_sides(
        gz, ngz, "gz",
        kext.at[pl.ds(4, 4)], kext.at[pl.ds(0, 4)],
        kext.at[pl.ds(nz, 4)], kext.at[pl.ds(nz + 4, 4)],
        kz_sem, zero,
    )

    for there, came in receives:
        if there is None:
            came.wait_recv()
        else:
            pl.when(there)(lambda came=came: came.wait_recv())

    tot = mz[0]
    for z in range(1, ngz):
        tot = tot + mz[z]
    scale = lax.rsqrt(tot[1:2, :] / (epochs * tot[2:3, :]) + EPS)

    def over_gz(ref, *index):
        value = ref[index + (0,)]
        for z in range(1, ngz):
            value = value + ref[index + (z,)]
        return value

    centre = over_gz(sc) * scale
    surf[:, HX:HX + lx, 0:LANES] = centre
    surf_out[...] = centre
    surf[:, 0:HX, 0:LANES] = over_gz(sx, 0) * scale
    surf[:, HX + lx:, 0:LANES] = over_gz(sx, 1) * scale
    edge_lane = (lane8 < 8) | (lane8 >= LANES - 8)
    for d in range(3):
        from_left = over_gz(sy, d, 0)
        from_right = over_gz(sy, d, 1)
        for c in range(3):
            for r in ((groups - 1,), range(groups), (0,))[d]:
                k = c * groups + r
                q, kk = k // 8, k % 8
                tile = jnp.where(
                    lane8 < 64, lane_roll(from_right[q], -16 * kk),
                    lane_roll(from_left[q], 112 - 16 * kk),
                )
                row = (0, HX + r * 8, HX + lx)[d]
                surf[c, row:row + 8, LANES:width] = jnp.where(edge_lane, tile * scale, 0.0)

    row_i = lax.broadcasted_iota(jnp.int32, (rows_x, width), 0)
    col_i = lax.broadcasted_iota(jnp.int32, (rows_x, width), 1)
    inside_x = ((row_i >= HX) | (gx > 0)) & ((row_i < HX + lx) | (gx < ngx - 1))
    inside_y = (col_i < LANES) | ((col_i < LANES + 8) & (gy < ngy - 1)) | (
        (col_i >= width - 8) & (gy > 0)
    )
    mask = jnp.where(inside_x & inside_y, 1.0, 0.0)

    for c in range(3):
        s = surf[c]
        fields[c] = (6.0 - SHIFT) * s - (up(s, 0) + down(s, 0)) - (up(s, 1) + down(s, 1))
    s0, s1, s2 = surf[0], surf[1], surf[2]
    flux = mask * 0.5 * ((up(s0, 0) - down(s0, 0)) + (up(s1, 1) - down(s1, 1)))
    fields[3] = flux
    fields[4] = 0.5 * (up(flux, 0) - down(flux, 0))
    fields[5] = 0.5 * (up(s2, 0) - down(s2, 0))
    fields[6] = 0.5 * (up(flux, 1) - down(flux, 1))
    fields[7] = 0.5 * (up(s2, 1) - down(s2, 1))
    fields[8] = mask

    z_all = nz * ngz

    def inside_z(z):
        return jnp.where((z >= 0) & (z < z_all), 1.0, 0.0).astype(F32)

    first_z = gz * nz

    def apply_first(iz, carry):
        zg = first_z + iz - 4
        dmm, dm, d0, dp, dpp = [dext[iz + j][0:1, 0:1] for j in range(5)]
        here = inside_z(zg)
        e0 = 0.5 * here * (dp - dm)
        ep = 0.5 * inside_z(zg + 1) * (dpp - d0)
        em = 0.5 * inside_z(zg - 1) * (d0 - dmm)
        k = kext[iz]
        m = fields[8] * here
        kd = k * d0 - (dm + dp)
        v1[0, iz] = m * (d0 * fields[0] + kd * surf[0]
                         - KAPPA * (d0 * fields[4] + e0 * fields[5]))
        v1[1, iz] = m * (d0 * fields[1] + kd * surf[1]
                         - KAPPA * (d0 * fields[6] + e0 * fields[7]))
        v1[2, iz] = m * (d0 * fields[2] + kd * surf[2]
                         - (0.5 * KAPPA) * ((dp - dm) * fields[3] + (ep - em) * surf[2]))
        return carry

    finish_z()
    lax.fori_loop(0, nz + 8, apply_first, 0, unroll=2)

    def again(source, planes, store):
        offset = (nz - planes) // 2

        def spread_of(iz, carry):
            zg = first_z + offset + iz - 1
            a = source[0, iz + 1]
            b = source[1, iz + 1]
            w = (up(a, 0) - down(a, 0)) + (up(b, 1) - down(b, 1))
            w = w + (source[2, iz + 2] - source[2, iz])
            div[iz] = (0.5 * inside_z(zg)) * fields[8] * w
            return carry

        lax.fori_loop(0, planes + 2, spread_of, 0, unroll=2)

        def image_of(iz, carry):
            zg = first_z + offset + iz
            k = kext[iz + offset + 4] + (6.0 - SHIFT)
            here = div[iz + 1]
            slopes = (
                up(here, 0) - down(here, 0),
                up(here, 1) - down(here, 1),
                div[iz + 2] - div[iz],
            )
            m = inside_z(zg) * fields[8]
            for c in range(3):
                a = source[c, iz + 2]
                near = (up(a, 0) + down(a, 0)) + (up(a, 1) + down(a, 1))
                near = near + (source[c, iz + 1] + source[c, iz + 3])
                store(c, iz, m * (k * a - near - (0.5 * KAPPA) * slopes[c]))
            return carry

        lax.fori_loop(0, planes, image_of, 0)

    def store2(c, iz, value):
        v2[c, iz] = value

    def store3(c, iz, value):
        v3[c, iz] = value[HX:HX + lx, 0:LANES]

    outs = [
        pltpu.make_async_copy(src, dst, out_sem.at[i])
        for i, (src, dst) in enumerate((
            (v1.at[:, pl.ds(4, nz), pl.ds(HX, lx), pl.ds(0, LANES)], v1_out),
            (v2.at[:, pl.ds(2, nz), pl.ds(HX, lx), pl.ds(0, LANES)], v2_out),
            (v3, v3_out),
        ))
    ]
    outs[0].start()
    again(v1, nz + 4, store2)
    outs[1].start()
    again(v2, nz, store3)
    outs[2].start()

    def fold(a):
        return jnp.sum(a.reshape(lx // 8, 8, LANES), axis=0)

    def products(iz, acc):
        d0 = dext[iz + 6][0:1, 0:1]
        acc = list(acc)
        for c in range(3):
            a0 = d0 * surf[c, HX:HX + lx, 0:LANES]
            a1 = v1[c, iz + 4, HX:HX + lx, 0:LANES]
            a2 = v2[c, iz + 2, HX:HX + lx, 0:LANES]
            a3 = v3[c, iz]
            for i, (a, b) in enumerate(
                ((a0, a0), (a0, a1), (a1, a1), (a1, a2), (a2, a2), (a2, a3))
            ):
                acc[i] = acc[i] + fold(a * b)
        return tuple(acc)

    acc = lax.fori_loop(0, nz, products, tuple([jnp.zeros((8, LANES), F32)] * 6), unroll=2)
    sub8 = lax.broadcasted_iota(jnp.int32, (8, LANES), 0)
    packed = jnp.zeros((8, LANES), F32)
    for i in range(6):
        packed = jnp.where(sub8 == i, jnp.sum(acc[i], axis=0, keepdims=True), packed)
    momsend[...] = packed
    mom[flat] = packed
    reduces = []
    for t in range(1, total):
        p, device = peer_of(t)
        q = lax.rem(flat + total - t, total)
        out = copy(momsend, mom.at[flat], r_send.at[t], r_recv.at[flat], device)
        out.start()
        reduces.append((out, copy(momsend, mom.at[q], r_send.at[t], r_recv.at[q], device)))
    for _, came in reduces:
        came.wait_recv()
    added = mom[0]
    for t in range(1, total):
        added = added + mom[t]
    mu = jnp.sum(added, axis=1, keepdims=True)
    mu = [jnp.broadcast_to(mu[i:i + 1, :], (1, LANES)) for i in range(6)]

    def inner(a, b):
        out = None
        for i, p in enumerate(a):
            for j, r in enumerate(b):
                if p is None or r is None:
                    continue
                term = p * r * mu[i + j]
                out = term if out is None else out + term
        return out

    def plus(a, factor, b):
        out = []
        for p, r in zip(a, b):
            if r is None:
                out.append(p)
            elif p is None:
                out.append(factor * r)
            else:
                out.append(p + factor * r)
        return out

    one = jnp.ones((1, LANES), F32)
    x = [None] * 4
    r = [one, None, None, None]
    p = [one, None, None, None]
    rr = mu[0]
    for step in range(ITERS):
        ap = [None] + p[:3]
        ap = plus(ap, SHIFT * one, p)
        alpha = rr / inner(p, ap)
        x = plus(x, alpha, p)
        r = plus(r, -alpha, ap)
        if step + 1 < ITERS:
            new = inner(r, r)
            p = plus(r, new / rr, p)
            rr = new
    rows = x[:3] + r
    result = jnp.zeros((8, LANES), F32)
    for i, value in enumerate(rows):
        result = jnp.where(sub8 == i, value, result)
    coef_out[...] = result

    for data, note, _, _ in exchange:
        data.wait_send()
        note.wait_send()
    for there, out in sends:
        if there is None:
            out.wait_send()
        else:
            pl.when(there)(lambda out=out: out.wait_send())
    for out, _ in reduces:
        out.wait_send()
    for out in outs:
        out.wait()

def combine(
    depth, coef, surf, v1_in, v2_in, v3_in, field_out, resid_out,
    v1, v2, v3, field, resid, in_sem, sem,
):
    nz = v1.shape[1]
    chunk = 4 if nz % 4 == 0 else 1
    arriving = []
    for start in range(0, nz, chunk):
        part = pl.ds(start, chunk)
        for i, (src, dst) in enumerate(((v1_in, v1), (v2_in, v2), (v3_in, v3))):
            load = pltpu.make_async_copy(
                src.at[:, part], dst.at[:, part], in_sem.at[i, start // chunk]
            )
            load.start()
            arriving.append(load)
    factors = [coef[i:i + 1, :] for i in range(7)]
    copies = []
    for start in range(0, nz, chunk):
        for load in arriving[3 * (start // chunk):3 * (start // chunk) + 3]:
            load.wait()
        for z in range(start, start + chunk):
            for c in range(3):
                a0 = depth[z] * surf[c]
                a1, a2 = v1[c, z], v2[c, z]
                field[c, z] = factors[0] * a0 + factors[1] * a1 + factors[2] * a2
                resid[c, z] = (factors[3] * a0 + factors[4] * a1) + (
                    factors[5] * a2 + factors[6] * v3[c, z]
                )
        part = pl.ds(start, chunk)
        for i, (src, dst) in enumerate(((field, field_out), (resid, resid_out))):
            out = pltpu.make_async_copy(
                src.at[:, part], dst.at[:, part], sem.at[i, start // chunk]
            )
            out.start()
            copies.append(out)
    for out in copies:
        out.wait()


def per_device(
    ngx, ngy, ngz,
    observed, predicted, coherence_mask, block_count, block_owner,
    block_matrix_choice, block_patch, look_vector, interp_weights, depth_kernel, stiffness,
):
    blocks, epochs, pixels = observed.shape
    owners = ngx * ngy
    total = owners * ngz
    cap = max(8, 2 * blocks // owners)
    nz, lx, ly = stiffness.shape
    rows_x = lx + 2 * HX
    width = 2 * LANES
    cells = PATCH_X * PATCH_Y
    meta_w = -(-owners * cap // LANES) * LANES
    packs = -(-3 * lx // 64)
    vmem = pl.BlockSpec(memory_space=pltpu.VMEM)
    smem = pl.BlockSpec(memory_space=pltpu.SMEM)
    hbm = pl.BlockSpec(memory_space=pltpu.HBM)
    dma = pltpu.SemaphoreType.DMA
    field = jax.ShapeDtypeStruct((3, nz, lx, ly), F32)

    def buf(*shape):
        return pltpu.VMEM(shape, F32)

    v1, v2, v3, surf, coef = pl.pallas_call(
        functools.partial(body, ngx, ngy, ngz, cap, epochs),
        out_shape=[field, field, field,
                   jax.ShapeDtypeStruct((3, lx, ly), F32),
                   jax.ShapeDtypeStruct((8, LANES), F32)],
        in_specs=[smem, smem, smem, vmem, vmem, vmem, vmem, hbm, hbm, hbm, hbm],
        out_specs=[hbm, hbm, hbm, vmem, vmem],
        scratch_shapes=[
            buf(blocks, epochs, pixels),
            buf(blocks, epochs, pixels),
            pltpu.VMEM(interp_weights.shape, BF16),
            buf(blocks, pixels),
            pltpu.VMEM((blocks, 8, pixels), BF16),
            dma((4,)),
            buf(blocks, 8, cells),
            buf(owners, 3 * cap, cells),
            buf(owners, 8, meta_w),
            buf(owners, 3 * cap, cells),
            buf(owners, 8, meta_w),
            buf(3, lx, ly),
            buf(2, packs, 8, LANES),
            buf(8, LANES),
            buf(2, ngz, 3, 8, LANES),
            buf(3, 2, ngz, packs, 8, LANES),
            buf(ngz, 3, lx, ly),
            buf(ngz, 8, LANES),
            buf(nz + 12, 8, LANES),
            buf(nz + 8, rows_x, width),
            buf(2, nz // 8, rows_x, LANES),
            buf(2, nz // 8, rows_x, LANES),
            buf(3, rows_x, width),
            buf(3, nz + 8, rows_x, width),
            buf(3, nz + 4, rows_x, width),
            buf(3, nz, lx, ly),
            buf(nz + 6, rows_x, width),
            buf(9, rows_x, width),
            buf(8, LANES),
            buf(total, 8, LANES),
            dma((owners,)), dma((owners,)), dma((owners,)), dma((owners,)),
            dma((4,)), dma((4,)), dma((4,)), dma((4,)),
            dma((2 * ngz + 8 * ngz,)),
            dma((2, ngz)), dma((3, 2, ngz)), dma((ngz,)), dma((ngz,)),
            dma((total,)), dma((total,)), dma((3,)),
        ],
        compiler_params=pltpu.CompilerParams(
            collective_id=0, has_side_effects=True, vmem_limit_bytes=VMEM_ALL
        ),
    )(
        block_matrix_choice, depth_kernel, look_vector, block_owner.reshape(1, blocks),
        block_patch[None, :], block_count[None, :], coherence_mask,
        observed, predicted, interp_weights, stiffness,
    )
    return pl.pallas_call(
        combine,
        out_shape=[field, field],
        in_specs=[smem, vmem, vmem, hbm, hbm, hbm],
        out_specs=[hbm, hbm],
        scratch_shapes=[buf(3, nz, lx, ly)] * 5 + [dma((3, nz)), dma((2, nz))],
        compiler_params=pltpu.CompilerParams(vmem_limit_bytes=VMEM_ALL),
    )(depth_kernel, coef, surf, v1, v2, v3)


def solution(mesh):
    spread = P(("grp", "gx", "gy", "gz"))
    in_specs = (
        P(("grp", "gx", "gy", "gz"), None, None),
        P(("grp", "gx", "gy", "gz"), None, None),
        P(("grp", "gx", "gy", "gz"), None),
        spread,
        P(("grp", "gx", "gy", "gz"), None),
        spread,
        spread,
        P(),
        P(),
        P(("grp", "gz")),
        P(("grp", "gz"), "gx", "gy"),
    )
    out_specs = (P(None, ("grp", "gz"), "gx", "gy"), P(None, ("grp", "gz"), "gx", "gy"))
    step = functools.partial(per_device, mesh.shape["gx"], mesh.shape["gy"], mesh.shape["gz"])
    return jax.shard_map(
        step, mesh=mesh, in_specs=in_specs, out_specs=out_specs, check_vma=False
    )
```
